8 devices in a mesh: dp: 1 (over z), tx: 2 (over y), ty: 4 (over x, core).
Axes of the slice: x: 2, y: 2, z: 1, core: 2. Of those that a mesh axis runs over, the one named last changes fastest.
Arguments:
- x_in: bfloat16 [64, 256, 1536], P('dp', None, 'tx')
- ln1_gain: float32 [2, 1536], P(None, 'tx')
- ln1_bias: float32 [2, 1536], P(None, 'tx')
- w_q: bfloat16 [2, 1536, 16, 96], P(None, 'tx', 'ty')
- b_q: float32 [2, 16, 96], P(None, 'ty')
- w_k: bfloat16 [2, 1536, 16, 96], P(None, 'tx', 'ty')
- w_v: bfloat16 [2, 1536, 16, 96], P(None, 'tx', 'ty')
- b_v: float32 [2, 16, 96], P(None, 'ty')
- w_o: bfloat16 [2, 16, 96, 1536], P(None, 'ty', None, 'tx')
- b_o: float32 [2, 1536], P(None, 'tx')
- ln2_gain: float32 [2, 1536], P(None, 'tx')
- ln2_bias: float32 [2, 1536], P(None, 'tx')
- w_up: bfloat16 [2, 1536, 6144], P(None, 'tx', 'ty')
- b_up: float32 [2, 6144], P(None, 'ty')
- w_down: bfloat16 [2, 6144, 1536], P(None, 'ty', 'tx')
- b_down: float32 [2, 1536], P(None, 'tx')
Outputs:
- output: bfloat16 [64, 256, 1536], P('dp', None, 'tx')
All inputs are finite; a program needn't handle non-finite values.
Results may differ from the reference program's by a relative error of at most 0.02.
Values are sent between devices in bfloat16 or wider.
A program may use at most 1 GiB of HBM per device.

```python
import jax
import jax.numpy as jnp
from jax import lax

IMGS = 64
N = 256
W = 1536
HEADS = 16
HEAD = 96
F = 6144
EPS = 1e-6


def setup_inputs(seed: int = 0, part: int = 0) -> dict:
    key = jax.random.key(seed)
    keys = jax.random.split(key, 16)
    act_keys = jax.random.split(jax.random.fold_in(key, part), 3)
    col_mean = 0.5 * jax.random.normal(act_keys[0], (W,), jnp.float32)
    col_scale = jnp.exp(0.5 * jax.random.normal(act_keys[1], (W,), jnp.float32))
    x_vals = jax.random.normal(act_keys[2], (IMGS, N, W), jnp.float32) * col_scale + col_mean
    w_scale = W ** -0.5
    f_scale = F ** -0.5

    def draw(index, shape, scale):
        return scale * jax.random.normal(keys[index], shape, jnp.float32)

    return {
        "x_in": x_vals.astype(jnp.bfloat16),
        "ln1_gain": 1.0 + draw(0, (2, W), 0.3),
        "ln1_bias": draw(1, (2, W), 0.3),
        "w_q": draw(2, (2, W, HEADS, HEAD), 1.7 * w_scale).astype(jnp.bfloat16),
        "b_q": draw(3, (2, HEADS, HEAD), 0.5),
        "w_k": draw(4, (2, W, HEADS, HEAD), 1.7 * w_scale).astype(jnp.bfloat16),
        "w_v": draw(5, (2, W, HEADS, HEAD), w_scale).astype(jnp.bfloat16),
        "b_v": draw(6, (2, HEADS, HEAD), 0.5),
        "w_o": draw(7, (2, HEADS, HEAD, W), w_scale).astype(jnp.bfloat16),
        "b_o": draw(8, (2, W), 0.3),
        "ln2_gain": 1.0 + draw(9, (2, W), 0.3),
        "ln2_bias": draw(10, (2, W), 0.3),
        "w_up": draw(11, (2, W, F), w_scale).astype(jnp.bfloat16),
        "b_up": draw(12, (2, F), 0.5),
        "w_down": draw(13, (2, F, W), f_scale).astype(jnp.bfloat16),
        "b_down": draw(14, (2, W), 0.3),
    }


def layer_norm(x_f, gain, shift):
    mean = jnp.mean(x_f, axis=-1, keepdims=True)
    centred = x_f - mean
    variance = jnp.mean(centred * centred, axis=-1, keepdims=True)
    return (centred * lax.rsqrt(variance + EPS) * gain + shift).astype(jnp.bfloat16)


def encoder_layer(x_img, params):
    (ln1_gain, ln1_bias, w_q, b_q, w_k, w_v, b_v, w_o, b_o,
     ln2_gain, ln2_bias, w_up, b_up, w_down, b_down) = params
    x_f = x_img.astype(jnp.float32)
    normed = layer_norm(x_f, ln1_gain, ln1_bias)
    q_proj = (jnp.dot(normed, w_q.reshape(W, W), preferred_element_type=jnp.float32) + b_q.reshape(W)).astype(jnp.bfloat16)
    k_proj = jnp.dot(normed, w_k.reshape(W, W), preferred_element_type=jnp.float32).astype(jnp.bfloat16)
    v_proj = (jnp.dot(normed, w_v.reshape(W, W), preferred_element_type=jnp.float32) + b_v.reshape(W)).astype(jnp.bfloat16)
    q_heads = q_proj.reshape(N, HEADS, HEAD).astype(jnp.float32)
    k_heads = k_proj.reshape(N, HEADS, HEAD).astype(jnp.float32)
    v_heads = v_proj.reshape(N, HEADS, HEAD).astype(jnp.float32)
    scores = jnp.einsum("qhd,khd->hqk", q_heads, k_heads) * (HEAD ** -0.5)
    attn_prob = jax.nn.softmax(scores, axis=-1).astype(jnp.bfloat16)
    attended = jnp.einsum("hqk,khd->qhd", attn_prob.astype(jnp.float32), v_heads).astype(jnp.bfloat16)
    x_mid = (x_f + jnp.dot(attended.reshape(N, W), w_o.reshape(W, W), preferred_element_type=jnp.float32) + b_o).astype(jnp.bfloat16)
    mid_f = x_mid.astype(jnp.float32)
    normed2 = layer_norm(mid_f, ln2_gain, ln2_bias)
    hidden = jax.nn.gelu(jnp.dot(normed2, w_up, preferred_element_type=jnp.float32) + b_up, approximate=True).astype(jnp.bfloat16)
    x_out = (mid_f + jnp.dot(hidden, w_down, preferred_element_type=jnp.float32) + b_down).astype(jnp.bfloat16)
    return x_out, None


def reference(x_in, ln1_gain, ln1_bias, w_q, b_q, w_k, w_v, b_v, w_o, b_o, ln2_gain, ln2_bias, w_up, b_up, w_down, b_down):
    params = (ln1_gain, ln1_bias, w_q, b_q, w_k, w_v, b_v, w_o, b_o,
              ln2_gain, ln2_bias, w_up, b_up, w_down, b_down)

    def run_image(x_img):
        x_last, _ = lax.scan(encoder_layer, x_img, params)
        return x_last

    return lax.map(run_image, x_in)
```

```python
import functools, math
import jax, jax.numpy as jnp
from jax import lax
from jax.experimental import pallas as pl
from jax.experimental.pallas import tpu as pltpu

EPS = 1e-6
F32 = jnp.float32
BF16 = jnp.bfloat16
TT = 512
NTOK = 256
HD = 96
GH = 4
GF = GH * HD
HW = 768
FB = 1536
ANY = pl.BlockSpec(memory_space=pl.ANY)
VM = pl.BlockSpec(memory_space=pltpu.VMEM)
NN = (((1,), (0,)), ((), ()))
NT = (((1,), (1,)), ((), ()))
TN = (((0,), (0,)), ((), ()))


def dot(a, b, dims=NN):
    return lax.dot_general(a, b, dims, preferred_element_type=F32)


def norm_into(x0_ref, x1_ref, gain_ref, shift_ref, h_ref, rows=64):
    @pl.loop(0, h_ref.shape[0] // rows)
    def _(i):
        at = pl.ds(pl.multiple_of(i * rows, rows), rows)
        a = x0_ref[at, :].astype(F32)
        b = x1_ref[at, :].astype(F32)
        width = 2.0 * HW
        mean = (jnp.sum(a, 1, keepdims=True) + jnp.sum(b, 1, keepdims=True)) / width
        a = a - mean
        b = b - mean
        var = (jnp.sum(a * a, 1, keepdims=True) + jnp.sum(b * b, 1, keepdims=True)) / width
        inv = lax.rsqrt(var + EPS)
        h_ref[at, :HW] = (a * inv * gain_ref[:, :HW] + shift_ref[:, :HW]).astype(BF16)
        h_ref[at, HW:] = (b * inv * gain_ref[:, HW:] + shift_ref[:, HW:]).astype(BF16)


def attention_kernel(x0_ref, x1_ref, gain_ref, shift_ref, bq_ref, bv_ref, bo_ref,
                     *rest):
    w = rest[:8]
    y0_ref, y1_ref, wqkv, wo, h_ref, qkv_ref, ot_ref, sems = rest[8:]
    step = pl.program_id(0)
    scale = HD ** -0.5 * math.log2(math.e)

    def loads(r):
        out = []
        for dy in range(2):
            src = w[dy * 4 + r]
            cols = slice(dy * HW, (dy + 1) * HW)
            out.append(pltpu.make_async_copy(src.at[0:3 * GF, :], wqkv.at[r, :, cols], sems.at[r, dy]))
            out.append(pltpu.make_async_copy(src.at[3 * GF:, :], wo.at[r * GF:(r + 1) * GF, cols], sems.at[r, 2 + dy]))
        return out

    @pl.when(step == 0)
    def _():
        for r in range(4):
            for c in loads(r):
                c.start()

    norm_into(x0_ref, x1_ref, gain_ref, shift_ref, h_ref)
    for r in range(4):
        @pl.when(step == 0)
        def _():
            for c in loads(r):
                c.wait()
        h = h_ref[...]
        at = slice(r * GF, (r + 1) * GF)
        qkv_ref[0:GF, :] = (dot(wqkv[r, 0:GF, :], h, NT) + bq_ref[at, :]).astype(BF16)
        qkv_ref[GF:2 * GF, :] = dot(wqkv[r, GF:2 * GF, :], h, NT).astype(BF16)
        qkv_ref[2 * GF:, :] = (dot(wqkv[r, 2 * GF:, :], h, NT) + bv_ref[at, :]).astype(BF16)
        for img in range(TT // NTOK):
            cols = slice(img * NTOK, (img + 1) * NTOK)
            for hd in range(GH):
                qt = qkv_ref[hd * HD:(hd + 1) * HD, cols]
                kt = qkv_ref[GF + hd * HD:GF + (hd + 1) * HD, cols]
                vt = qkv_ref[2 * GF + hd * HD:2 * GF + (hd + 1) * HD, cols]
                st = dot(kt, qt, TN)
                top = jnp.max(st, 0, keepdims=True)
                e = jnp.exp2((st - top) * scale)
                p = (e * (1.0 / jnp.sum(e, 0, keepdims=True))).astype(BF16)
                ot_ref[r * GF + hd * HD:r * GF + (hd + 1) * HD, cols] = dot(vt, p).astype(BF16)
    o = ot_ref[...].T
    y0_ref[...] = (x0_ref[...].astype(F32) + dot(o, wo[:, :HW]) + bo_ref[:, :HW]).astype(BF16)
    y1_ref[...] = (x1_ref[...].astype(F32) + dot(o, wo[:, HW:]) + bo_ref[:, HW:]).astype(BF16)


def attention(x0, x1, gain, shift, bq, bv, bo, w):
    t = x0.shape[0]
    blk = pl.BlockSpec((TT, HW), lambda i: (i, 0))
    out = jax.ShapeDtypeStruct((t, HW), BF16)
    return pl.pallas_call(
        attention_kernel, grid=(t // TT,), out_shape=(out, out),
        in_specs=[blk, blk] + [VM] * 5 + [ANY] * 8, out_specs=(blk, blk),
        scratch_shapes=[pltpu.VMEM((4, 3 * GF, 2 * HW), BF16), pltpu.VMEM((4 * GF, 2 * HW), BF16),
                        pltpu.VMEM((TT, 2 * HW), BF16), pltpu.VMEM((3 * GF, TT), BF16),
                        pltpu.VMEM((4 * GF, TT), BF16), pltpu.SemaphoreType.DMA((4, 4))],
        compiler_params=pltpu.CompilerParams(vmem_limit_bytes=60 << 20),
        cost_estimate=pl.CostEstimate(flops=t * 2 * 1536 * (4 * 1536 + 2 * 256), bytes_accessed=32 << 20, transcendentals=t * 16 * 256),
        name="attention",
    )(x0, x1, gain, shift, bq, bv, bo, *w)


def gelu(x):
    return 0.5 * x * (1.0 + jnp.tanh(x * (0.7978845608028654 + 0.035677408136300125 * (x * x))))


def up_kernel(x0_ref, x1_ref, gain_ref, shift_ref, b_ref, *rest):
    w = rest[:8]
    u_ref, ws, h_ref, sems = rest[8:]
    step = pl.program_id(0)

    def loads(r):
        return [pltpu.make_async_copy(w[dy * 4 + r], ws.at[r, dy * HW:(dy + 1) * HW, :], sems.at[r, dy]) for dy in range(2)]

    @pl.when(step == 0)
    def _():
        for r in range(4):
            for c in loads(r):
                c.start()
    norm_into(x0_ref, x1_ref, gain_ref, shift_ref, h_ref)
    for r in range(4):
        @pl.when(step == 0)
        def _():
            for c in loads(r):
                c.wait()
        nb = 512
        for j in range(FB // nb):
            cols = slice(j * nb, (j + 1) * nb)
            t = dot(h_ref[...], ws[r, :, cols]) + b_ref[r:r + 1, cols]
            u_ref[:, r * FB + j * nb: r * FB + (j + 1) * nb] = gelu(t).astype(BF16)


def up(x0, x1, gain, shift, b, w):
    t = x0.shape[0]
    blk = pl.BlockSpec((TT, HW), lambda i: (i, 0))
    return pl.pallas_call(
        up_kernel, grid=(t // TT,), out_shape=jax.ShapeDtypeStruct((t, 4 * FB), BF16),
        in_specs=[blk, blk] + [VM] * 3 + [ANY] * 8, out_specs=pl.BlockSpec((TT, 4 * FB), lambda i: (i, 0)),
        scratch_shapes=[pltpu.VMEM((4, 2 * HW, FB), BF16), pltpu.VMEM((TT, 2 * HW), BF16), pltpu.SemaphoreType.DMA((4, 2))],
        compiler_params=pltpu.CompilerParams(vmem_limit_bytes=60 << 20),
        cost_estimate=pl.CostEstimate(flops=t * 2 * 1536 * 6144, bytes_accessed=50 << 20, transcendentals=t * 6144),
        name="up",
    )(x0, x1, gain, shift, b, *w)


def down_kernel(u_ref, x0_ref, x1_ref, b_ref, *rest):
    w = rest[:8]
    y0_ref, y1_ref, ws, sems = rest[8:]
    step = pl.program_id(0)

    def loads(r):
        return [pltpu.make_async_copy(w[dy * 4 + r], ws.at[r * FB:(r + 1) * FB, dy * HW:(dy + 1) * HW], sems.at[r, dy]) for dy in range(2)]

    @pl.when(step == 0)
    def _():
        for r in range(4):
            for c in loads(r):
                c.start()
        for r in range(4):
            for c in loads(r):
                c.wait()
    nb = 768
    for j in range(HW // nb):
        cols = slice(j * nb, (j + 1) * nb)
        y0_ref[:, cols] = (x0_ref[:, cols].astype(F32) + dot(u_ref[...], ws[:, cols]) + b_ref[:, cols]).astype(BF16)
    for j in range(HW // nb):
        cols = slice(j * nb, (j + 1) * nb)
        c2 = slice(HW + j * nb, HW + (j + 1) * nb)
        y1_ref[:, cols] = (x1_ref[:, cols].astype(F32) + dot(u_ref[...], ws[:, c2]) + b_ref[:, c2]).astype(BF16)


def down(u, x0, x1, b, w):
    t = x0.shape[0]
    blk = pl.BlockSpec((TT, HW), lambda i: (i, 0))
    out = jax.ShapeDtypeStruct((t, HW), BF16)
    return pl.pallas_call(
        down_kernel, grid=(t // TT,), out_shape=(out, out),
        in_specs=[pl.BlockSpec((TT, 4 * FB), lambda i: (i, 0)), blk, blk, VM] + [ANY] * 8, out_specs=(blk, blk),
        scratch_shapes=[pltpu.VMEM((4 * FB, 2 * HW), BF16), pltpu.SemaphoreType.DMA((4, 2))],
        compiler_params=pltpu.CompilerParams(vmem_limit_bytes=60 << 20),
        cost_estimate=pl.CostEstimate(flops=t * 2 * 1536 * 6144, bytes_accessed=50 << 20, transcendentals=0),
        name="down",
    )(u, x0, x1, b, *w)
from jax.sharding import PartitionSpec as P


def solution(mesh):
    tx_size, ty_size = mesh.shape["tx"], mesh.shape["ty"]
    axes = ("tx", "ty")
    devices = tx_size * ty_size
    act_spec = P("dp", None, "tx")
    vec_tx = P(None, "tx")
    proj_spec = P(None, "tx", "ty", None)
    head_vec = P(None, "ty", None)
    in_specs = (act_spec, vec_tx, vec_tx, proj_spec, head_vec, proj_spec, proj_spec, head_vec,
                P(None, "ty", None, "tx"), vec_tx, vec_tx, vec_tx,
                P(None, "tx", "ty"), P(None, "ty"), P(None, "ty", "tx"), vec_tx)

    def swap(a, bits):
        return lax.ppermute(a, axes, [(i, i ^ bits) for i in range(devices)])

    Y, X, C = 4, 2, 1

    def gather(own, relay_on_x, after):
        if after is not None:
            own, _ = lax.optimization_barrier((own, after))
        px, py = swap(own, X), swap(own, Y)
        pxy = swap(py, X) if relay_on_x else swap(px, Y)
        quads = [own, px, py, pxy]
        other = [swap(a, C) for a in quads]
        return [quads[0], other[0], quads[1], other[1], quads[2], other[2], quads[3], other[3]]

    def local_fn(x_in, ln1_gain, ln1_bias, w_q, b_q, w_k, w_v, b_v, w_o, b_o, ln2_gain, ln2_bias, w_up, b_up, w_down, b_down):
        layers = w_q.shape[0]
        me = lax.axis_index("tx") * ty_size + lax.axis_index("ty")
        imgs = x_in.shape[0] // devices
        mine = lax.dynamic_slice_in_dim(x_in, me * imgs, imgs, 0).reshape(-1, HW)
        theirs = lax.dynamic_slice_in_dim(x_in, jnp.bitwise_xor(me, Y) * imgs, imgs, 0).reshape(-1, HW)
        x0, x1 = mine, swap(theirs, Y)
        vec = jnp.stack([ln1_gain, ln1_bias, b_o, ln2_gain, ln2_bias, b_down], 1)
        vec = jnp.concatenate([vec, swap(vec, Y)], -1)
        hid = jnp.concatenate([b_q.reshape(layers, GF), b_v.reshape(layers, GF), b_up], -1)
        hx = swap(hid, X)
        hid = jnp.stack([hid, swap(hid, C), hx, swap(hx, C)], 1)

        def heads_first(w):
            return jnp.transpose(w, (0, 2, 3, 1)).reshape(layers, GF, HW)
        wa = jnp.concatenate([heads_first(w_q), heads_first(w_k), heads_first(w_v), w_o.reshape(layers, GF, HW)], 1)
        relay = iter((True, True, False, True, False, False))
        for layer in range(layers):
            v = vec[layer]
            h = hid[layer]
            ga = gather(wa[layer], next(relay), (x1 if layer == 0 else (gd0[2], gd0[4])))
            x0, x1 = attention(x0, x1, v[0:1], v[1:2], h[:, :GF].reshape(-1, 1), h[:, GF:2 * GF].reshape(-1, 1), v[2:3], ga)
            gu = gather(w_up[layer], next(relay), (ga[2], ga[4]))
            u = up(x0, x1, v[3:4], v[4:5], h[:, 2 * GF:], gu)
            gd = gd0 = gather(w_down[layer], next(relay), (gu[2], gu[4]))
            x0, x1 = down(u, x0, x1, v[5:6], gd)
        got = [x0, swap(x1, Y)]
        got = [got[0], swap(got[0], X), got[1], swap(got[1], X)]
        got = [a for g in got for a in (g, swap(g, C))]
        out = jnp.zeros_like(x_in)
        for bits, a in zip((0, C, X, X | C, Y, Y | C, Y | X, Y | X | C), got):
            at = jnp.bitwise_xor(me, bits) * imgs
            out = lax.dynamic_update_slice_in_dim(out, a.reshape(imgs, NTOK, HW), at, 0)
        return out

    return jax.shard_map(local_fn, mesh=mesh, in_specs=in_specs, out_specs=act_spec, check_vma=False)
```

```python
import math

import jax
import jax.numpy as jnp
from jax import lax
from jax.experimental import pallas as pl
from jax.experimental.pallas import tpu as pltpu
from jax.sharding import PartitionSpec as P

EPS = 1e-6
F32 = jnp.float32
BF16 = jnp.bfloat16
MESH = pl.DeviceIdType.MESH

IMGS = 8
NTOK = 256
TILES = 4
TT = 512
HD = 96
GH = 4
GF = GH * HD
HW = 768
FB = 1536
UC = 384
DC = 256
NA, NU, ND = 4, 4, 3
PER_LAYER = NA + NU + ND
LAYERS = 2
CHUNKS = LAYERS * PER_LAYER
UNITS = ND * TILES

X, Y, C = 2, 4, 1
XC, YC, XY, XYC = 3, 5, 6, 7

NN = (((1,), (0,)), ((), ()))
NT = (((1,), (1,)), ((), ()))
TN = (((0,), (0,)), ((), ()))


def dot(a, b, dims=NN):
    return lax.dot_general(a, b, dims, preferred_element_type=F32)


def gelu(x):
    return 0.5 * x * (1.0 + jnp.tanh(x * (0.7978845608028654 + 0.035677408136300125 * (x * x))))


def chunk_kind(k):
    layer, j = divmod(k, PER_LAYER)
    if j < NA:
        return layer, "a", j
    if j < NA + NU:
        return layer, "u", j - NA
    return layer, "d", j - NA - NU


def relay_on_x(k):
    layer, kind, j = chunk_kind(k)
    return (layer, kind) in ((0, "a"), (0, "u"), (1, "a"))


LINK = 45.5e3
LOOK = 3
T_ATT, T_UP, T_DOWN = 6.0, 3.3, 4.3


def chunk_bytes(k):
    return 2 * (FB * DC if chunk_kind(k)[1] == "d" else GF * HW)


def plan():
    free = {"x": 0.0, "y": 0.0, "c": 0.0}
    ready = {}
    pending = []
    program = []
    now = [0.0]

    def send(link, size, lag=2.5):
        rate = 450e3 if link == "c" else LINK
        start = max(free[link], now[0])
        free[link] = start + size / rate
        return free[link] + lag

    def arrive(name, time, action=None, rank=1):
        ready[name] = time
        if action is not None:
            pending.append((time, rank, action))

    def do(action):
        program.append(("do", action))
        kind = action[0]
        if kind == "ownx":
            arrive(("w", X, action[1]), send("x", chunk_bytes(action[1])), ("gotx", action[1]), 2)
        elif kind == "owny":
            arrive(("w", Y, action[1]), send("y", chunk_bytes(action[1])), ("goty", action[1]))
        elif kind == "ownc":
            arrive(("w", C, action[1]), send("c", chunk_bytes(action[1])))
        elif kind == "image":
            arrive(("image", action[1]), send("y", NTOK * HW * 2))
        elif kind == "gotx":
            k = action[1]
            arrive(("w", XC, k), send("c", chunk_bytes(k)))
            if not relay_on_x(k):
                arrive(("w", XY, k), send("y", chunk_bytes(k)), ("gotd", k))
            if k >= LOOK and k + LOOK < CHUNKS:
                do(("ownx", k + LOOK))
            if k == LOOK - 1:
                for j in range(LOOK, 2 * LOOK):
                    do(("ownx", j))
        elif kind == "goty":
            k = action[1]
            arrive(("w", YC, k), send("c", chunk_bytes(k)))
            if relay_on_x(k):
                arrive(("w", XY, k), send("x", chunk_bytes(k)), ("gotd", k))
            if k + LOOK < CHUNKS:
                do(("owny", k + LOOK))
                do(("ownc", k + LOOK))
        elif kind == "gotd":
            arrive(("w", XYC, action[1]), send("c", chunk_bytes(action[1])))
        elif kind == "out":
            size = TT * DC * 2
            q = action[1]
            arrive(("o", X, q), send("x", size), ("outx", q), 2)
            arrive(("o", Y, q), send("y", size), ("outy", q))
            arrive(("o", C, q), send("c", size))
        elif kind == "outx":
            arrive(("o", XC, action[1]), send("c", TT * DC * 2))
        elif kind == "outy":
            arrive(("o", XY, action[1]), send("x", TT * DC * 2), ("outd", action[1]))
            arrive(("o", YC, action[1]), send("c", TT * DC * 2))
        elif kind == "outd":
            arrive(("o", XYC, action[1]), send("c", TT * DC * 2))

    def pump():
        while True:
            due = [p for p in pending if p[0] <= now[0]]
            if not due:
                return
            first = min(due, key=lambda p: (p[0], p[1]))
            pending.remove(first)
            do(first[2])

    def block(layer, kind, n, needs, cost):
        while True:
            pump()
            late = [ready.get(a, 1e9) for a in needs if ready.get(a, 1e9) > now[0]]
            if not late and all(a in ready for a in needs):
                break
            times = [p[0] for p in pending] + [t for t in late if t < 1e9]
            now[0] = max(now[0], min(times))
        program.append(("block", layer, kind, n))
        now[0] += cost

    do(("small",))
    for k in range(LOOK):
        do(("ownx", k))
        do(("owny", k))
        do(("ownc", k))
    for i in range(IMGS):
        do(("image", i))

    def whole(k):
        return [("w", s, k) for s in (X, Y, C, XC, YC, XY, XYC)]

    for layer in range(LAYERS):
        base = layer * PER_LAYER
        for n in range(4 * TILES):
            needs = [a for k in range(NA - 1) for a in whole(base + k)]
            if n % 4 == 3:
                needs += whole(base + NA - 1)
            if layer == 0:
                needs += [("image", i) for i in range(2 * (n // 4) + 2)]
            block(layer, "a", n, needs, T_ATT)
        for n in range(NU * TILES):
            block(layer, "u", n, whole(base + NA + n // TILES), T_UP)
        for n in range(ND * TILES):
            block(layer, "d", n, whole(base + NA + NU + n // TILES), T_DOWN)
            if layer == LAYERS - 1 and n >= 1:
                do(("out", n - 1))
    do(("out", UNITS - 1))
    while pending:
        now[0] = max(now[0], min(p[0] for p in pending))
        pump()
    return program, max(now[0], max(ready.values()))


def mega_kernel(x_in, wq, wk, wv, wo, wup, wdown, vec_own, hid_own,
                y_out, land_a, land_u, land_d,
                x0, x1, h, u, ubuf, dbuf, vec_oth, hid,
                wsend, wrecv, isend, irecv, osend, orecv, small_send, small_recv,
                local_sem, asem, usem, dsem):
    ty, tx = lax.axis_index("ty"), lax.axis_index("tx")
    core, xx = lax.rem(ty, 2), ty // 2
    me = tx * 4 + ty
    over_x = {"ty": (1 - xx) * 2 + core}
    over_y = {"tx": 1 - tx}
    over_c = {"ty": xx * 2 + (1 - core)}
    place = {X: tx * 4 + (1 - xx) * 2 + core, Y: (1 - tx) * 4 + ty, XY: (1 - tx) * 4 + (1 - xx) * 2 + core, 0: me}
    other = {s: p + 1 - 2 * core for s, p in place.items()}
    place.update({s + 1: p for s, p in other.items()})
    src_wa = (wq, wk, wv, wo)

    barrier = pltpu.get_barrier_semaphore()
    for peer in (over_x, over_y, over_c):
        pl.semaphore_signal(barrier, inc=1, device_id=peer, device_id_type=MESH)
    pl.semaphore_wait(barrier, 3)

    def remote(src, dst, send, recv, peer):
        return pltpu.make_async_remote_copy(src_ref=src, dst_ref=dst, send_sem=send, recv_sem=recv,
                                            device_id=peer, device_id_type=MESH)

    def own_ref(k):
        layer, kind, j = chunk_kind(k)
        if kind == "a":
            return src_wa[j].at[layer]
        if kind == "u":
            return wup.at[layer, :, j * UC:(j + 1) * UC]
        return wdown.at[layer, :, j * DC:(j + 1) * DC]

    def land_ref(k, s):
        layer, kind, j = chunk_kind(k)
        if kind == "a":
            return land_a.at[layer, s - 1, j * GF:(j + 1) * GF, :]
        if kind == "u":
            return land_u.at[layer, s - 1, :, j * UC:(j + 1) * UC]
        return land_d.at[layer, s - 1, :, j * DC:(j + 1) * DC]

    def weight_copy(k, s):
        if s == X:
            src, peer = own_ref(k), over_x
        elif s == Y:
            src, peer = own_ref(k), over_y
        elif s == C:
            src, peer = own_ref(k), over_c
        elif s == XY:
            src, peer = (land_ref(k, Y), over_x) if relay_on_x(k) else (land_ref(k, X), over_y)
        else:
            src, peer = land_ref(k, s - 1), over_c
        return remote(src, land_ref(k, s), wsend.at[k, s - 1], wrecv.at[k, s - 1], peer)

    def image_copy(i):
        theirs = (1 - tx) * 4 + ty
        return remote(x_in.at[theirs * IMGS + i], x1.at[i], isend.at[i], irecv.at[i], over_y)

    def out_ref(slot, q):
        cc, i = divmod(q, TILES)
        return y_out.at[pl.ds(place[slot] * IMGS + 2 * i, 2), :, cc * DC:(cc + 1) * DC]

    def out_copy(q, s):
        cc, i = divmod(q, TILES)
        cols = slice(cc * DC, (cc + 1) * DC)
        rows = slice(2 * i, 2 * i + 2)
        if s == X:
            src, dst, peer = x0.at[rows, :, cols], out_ref(0, q), over_x
        elif s == C:
            src, dst, peer = x0.at[rows, :, cols], out_ref(0, q), over_c
        elif s == Y:
            src, dst, peer = x1.at[rows, :, cols], out_ref(0, q), over_y
        elif s == XY:
            src, dst, peer = out_ref(Y, q), out_ref(Y, q), over_x
        else:
            src, dst, peer = out_ref(s - 1, q), out_ref(s - 1, q), over_c
        return remote(src, dst, osend.at[q, s - 1], orecv.at[q, s - 1], peer)

    def keep_copy(q):
        cc, i = divmod(q, TILES)
        return pltpu.make_async_copy(x0.at[2 * i:2 * i + 2, :, cc * DC:(cc + 1) * DC], out_ref(0, q), dsem.at[2, q])

    def out_arrived(q, s):
        return remote(out_ref(s, q), out_ref(s, q), osend.at[q, s - 1], orecv.at[q, s - 1], over_x)

    vec_copy = remote(vec_own, vec_oth, small_send.at[0], small_recv.at[0], over_y)
    hid_x = remote(hid_own, hid.at[X], small_send.at[1], small_recv.at[1], over_x)
    hid_c = remote(hid_own, hid.at[C], small_send.at[2], small_recv.at[2], over_c)
    hid_xc = remote(hid.at[X], hid.at[XC], small_send.at[3], small_recv.at[3], over_c)
    own_rows = pltpu.make_async_copy(x_in.at[pl.ds(me * IMGS, IMGS)], x0, local_sem.at[0])
    own_hid = pltpu.make_async_copy(hid_own, hid.at[0], local_sem.at[1])

    def act(action):
        kind, *k = action
        k = k[0] if k else None
        if kind == "small":
            vec_copy.start()
            hid_x.start()
            hid_c.start()
            own_rows.start()
            own_hid.start()
        elif kind == "ownx":
            weight_copy(k, X).start()
        elif kind == "owny":
            weight_copy(k, Y).start()
        elif kind == "ownc":
            weight_copy(k, C).start()
        elif kind == "image":
            image_copy(k).start()
        elif kind == "gotx":
            weight_copy(k, X).wait_recv()
            if not relay_on_x(k):
                weight_copy(k, XY).start()
            weight_copy(k, XC).start()
        elif kind == "goty":
            weight_copy(k, Y).wait_recv()
            if relay_on_x(k):
                weight_copy(k, XY).start()
            weight_copy(k, YC).start()
        elif kind == "gotd":
            weight_copy(k, XY).wait_recv()
            weight_copy(k, XYC).start()
        elif kind == "out":
            for s in (X, Y, C):
                out_copy(k, s).start()
            keep_copy(k).start()
        elif kind == "outx":
            out_arrived(k, X).wait_recv()
            out_copy(k, XC).start()
        elif kind == "outy":
            out_arrived(k, Y).wait_recv()
            out_copy(k, XY).start()
            out_copy(k, YC).start()
        elif kind == "outd":
            out_arrived(k, XY).wait_recv()
            out_copy(k, XYC).start()

    def slot_ref(land, own, layer, s):
        return own.at[layer] if s == 0 else land.at[layer, s - 1]

    def a_loads(layer, r):
        out = []
        for dy in range(2):
            s = dy * 4 + r
            cols = slice(r * 2 * HW + dy * HW, r * 2 * HW + (dy + 1) * HW)
            if s == 0:
                for j in range(3):
                    out.append((src_wa[j].at[layer], u.at[j * GF:(j + 1) * GF, cols], asem.at[s, j]))
            else:
                out.append((land_a.at[layer, s - 1, 0:3 * GF, :], u.at[0:3 * GF, cols], asem.at[s, 0]))
        return [pltpu.make_async_copy(*c) for c in out]

    def o_loads(layer):
        out = []
        for r in range(4):
            for dy in range(2):
                s = dy * 4 + r
                src = wo.at[layer] if s == 0 else land_a.at[layer, s - 1, 3 * GF:4 * GF, :]
                at = 3 * GF + (r % 2) * GF
                cols = slice((r // 2) * 2 * HW + dy * HW, (r // 2) * 2 * HW + (dy + 1) * HW)
                out.append(pltpu.make_async_copy(src, u.at[at:at + GF, cols], asem.at[s, 3]))
        return out

    def u_loads(layer, k):
        b = k % 2
        out = []
        for r in range(4):
            for dy in range(2):
                s = dy * 4 + r
                src = slot_ref(land_u, wup, layer, s).at[:, k * UC:(k + 1) * UC]
                out.append(pltpu.make_async_copy(
                    src, ubuf.at[b, dy * HW:(dy + 1) * HW, r * UC:(r + 1) * UC], usem.at[b, s]))
        return out

    def d_loads(layer, cc):
        b = cc % 2
        out = []
        for r in range(4):
            for dy in range(2):
                s = dy * 4 + r
                src = slot_ref(land_d, wdown, layer, s).at[:, cc * DC:(cc + 1) * DC]
                out.append(pltpu.make_async_copy(
                    src, dbuf.at[b, r * FB:(r + 1) * FB, dy * DC:(dy + 1) * DC], dsem.at[b, s]))
        return out

    def start(copies):
        for c in copies:
            c.start()

    def finish(copies):
        for c in copies:
            c.wait()

    def arrived(k):
        for s in (C, XC, YC, XYC):
            weight_copy(k, s).wait_recv()

    def vec_row(layer, j):
        at = slice(layer * 6 + j, layer * 6 + j + 1)
        return vec_own[at, :], vec_oth[at, :]

    def norm(layer, j, tile):
        g0, g1 = vec_row(layer, j)
        s0, s1 = vec_row(layer, j + 1)
        rows = 64

        @pl.loop(0, TT // rows)
        def _(i):
            img = 2 * tile + i // (NTOK // rows)
            at = pl.ds(pl.multiple_of(lax.rem(i, NTOK // rows) * rows, rows), rows)
            a = x0[img, at, :].astype(F32)
            b = x1[img, at, :].astype(F32)
            width = 2.0 * HW
            mean = (jnp.sum(a, 1, keepdims=True) + jnp.sum(b, 1, keepdims=True)) / width
            a = a - mean
            b = b - mean
            var = (jnp.sum(a * a, 1, keepdims=True) + jnp.sum(b * b, 1, keepdims=True)) / width
            inv = lax.rsqrt(var + EPS)
            to = pl.ds(pl.multiple_of(tile * TT + i * rows, rows), rows)
            h[to, :HW] = (a * inv * g0 + s0).astype(BF16)
            h[to, HW:] = (b * inv * g1 + s1).astype(BF16)

    scale = HD ** -0.5 * math.log2(math.e)
    qkv = dbuf.at[0, 4 * GF:7 * GF, :]
    ot = dbuf.at[0, 0:4 * GF, :]

    def column(layer, r, at):
        row = hid[r, layer:layer + 1, at:at + GF]
        col = jnp.broadcast_to(row, (128, GF)).T
        return jnp.concatenate([col] * (TT // 128), 1)

    def attention_block(layer, tile, r):
        rows = pl.ds(pl.multiple_of(tile * TT, TT), TT)
        cols = pl.ds(pl.multiple_of(r * 2 * HW, 2 * HW), 2 * HW)
        hh = h[rows, :]
        qkv[0:GF, :] = (dot(u[0:GF, cols], hh, NT) + column(layer, r, 0)).astype(BF16)
        qkv[GF:2 * GF, :] = dot(u[GF:2 * GF, cols], hh, NT).astype(BF16)
        qkv[2 * GF:3 * GF, :] = (dot(u[2 * GF:3 * GF, cols], hh, NT) + column(layer, r, GF)).astype(BF16)
        for img in range(TT // NTOK):
            c = slice(img * NTOK, (img + 1) * NTOK)
            for hd in range(GH):
                qt = qkv[hd * HD:(hd + 1) * HD, c]
                kt = qkv[GF + hd * HD:GF + (hd + 1) * HD, c]
                vt = qkv[2 * GF + hd * HD:2 * GF + (hd + 1) * HD, c]
                st = dot(kt, qt, TN)
                top = jnp.max(st, 0, keepdims=True)
                e = jnp.exp2((st - top) * scale)
                p = (e * (1.0 / jnp.sum(e, 0, keepdims=True))).astype(BF16)
                ot[pl.ds(pl.multiple_of(r * GF, GF) + hd * HD, HD), c] = dot(vt, p).astype(BF16)

    def project_block(layer, tile):
        b0, b1 = vec_row(layer, 2)
        o = ot[...].T
        imgs = pl.ds(2 * tile, 2)
        for half, ref, bias in ((0, x0, b0), (1, x1, b1)):
            acc = dot(o[:, :HW], u[3 * GF:5 * GF, half * HW:(half + 1) * HW])
            acc += dot(o[:, HW:], u[3 * GF:5 * GF, 2 * HW + half * HW:2 * HW + (half + 1) * HW])
            old = ref[imgs].reshape(TT, HW).astype(F32)
            ref[imgs] = (old + acc + bias).astype(BF16).reshape(2, NTOK, HW)

    def up_block(layer, k, tile, b):
        rows = pl.ds(pl.multiple_of(tile * TT, TT), TT)
        for nb in range(2):
            bias = jnp.concatenate(
                [hid[2 * nb + j, layer:layer + 1, pl.ds(pl.multiple_of(2 * GF + k * UC, 128), UC)] for j in range(2)], 1)
            t = gelu(dot(h[rows, :], ubuf[b, :, nb * 2 * UC:(nb + 1) * 2 * UC]) + bias).astype(BF16)
            for j in range(2):
                u[rows, pl.ds(pl.multiple_of((2 * nb + j) * FB + k * UC, 128), UC)] = t[:, j * UC:(j + 1) * UC]

    def down_block(layer, cc, tile, b):
        rows = pl.ds(pl.multiple_of(tile * TT, TT), TT)
        imgs = pl.ds(2 * tile, 2)
        cols = pl.ds(pl.multiple_of(cc * DC, DC), DC)
        at = layer * 6 + 5
        acc = dot(u[rows, :], dbuf[b])
        for half, ref, vec in ((0, x0, vec_own), (1, x1, vec_oth)):
            old = ref[imgs, :, cols].reshape(TT, DC).astype(F32)
            new = old + acc[:, half * DC:(half + 1) * DC] + vec[at:at + 1, cols]
            ref[imgs, :, cols] = new.astype(BF16).reshape(2, NTOK, DC)

    program, _ = plan()
    before = {}
    todo = []
    tail = []
    for item in program:
        if item[0] == "do":
            todo.append(item[1])
        else:
            before[item[1:]] = todo
            todo = []
    tail = todo

    def ahead(layer, kind, n, count):
        for m in range(count):
            actions = before[(layer, kind, m)]
            if actions and not (layer == 0 and kind == "a" and m == 0):
                @pl.when(n == m)
                def _(actions=actions):
                    for a in actions:
                        act(a)

    for a in before[(0, "a", 0)]:
        act(a)
    hid_x.wait_recv()
    hid_xc.start()
    hid_c.wait_recv()
    hid_xc.wait_recv()
    vec_copy.wait_recv()
    own_rows.wait()
    own_hid.wait()

    for layer in range(LAYERS):
        base = layer * PER_LAYER

        @pl.loop(0, 4 * TILES)
        def _(n, layer=layer, base=base):
            ahead(layer, "a", n, 4 * TILES)
            tile, r = n // 4, lax.rem(n, 4)

            @pl.when(n == 0)
            def _():
                for k in range(NA - 1):
                    arrived(base + k)
                for q in range(4):
                    start(a_loads(layer, q))

            @pl.when(n == 3)
            def _():
                arrived(base + NA - 1)
                start(o_loads(layer))

            for q in range(4):
                @pl.when(n == q)
                def _(q=q):
                    finish(a_loads(layer, q))

            @pl.when(r == 0)
            def _():
                if layer == 0:
                    for i in range(TILES):
                        @pl.when(tile == i)
                        def _(i=i):
                            image_copy(2 * i).wait_recv()
                            image_copy(2 * i + 1).wait_recv()
                norm(layer, 0, tile)
            attention_block(layer, tile, r)

            @pl.when(n == 3)
            def _():
                finish(o_loads(layer))

            @pl.when(r == 3)
            def _():
                project_block(layer, tile)
                norm(layer, 3, tile)

        @pl.loop(0, NU * TILES)
        def _(n, layer=layer, base=base):
            ahead(layer, "u", n, NU * TILES)
            k, tile = n // TILES, lax.rem(n, TILES)
            b = lax.rem(k, 2)
            for j in range(NU):
                @pl.when(n == j * TILES)
                def _(j=j):
                    arrived(base + NA + j)
                    start(u_loads(layer, j))
                    finish(u_loads(layer, j))
            up_block(layer, k, tile, b)

        @pl.loop(0, ND * TILES)
        def _(n, layer=layer, base=base):
            ahead(layer, "d", n, ND * TILES)
            cc, tile = n // TILES, lax.rem(n, TILES)
            b = lax.rem(cc, 2)
            for j in range(ND):
                @pl.when(n == j * TILES)
                def _(j=j):
                    arrived(base + NA + NU + j)
                    start(d_loads(layer, j))
                    finish(d_loads(layer, j))
            down_block(layer, cc, tile, b)

    for a in tail:
        act(a)
    for q in range(UNITS):
        keep_copy(q).wait()
        for s in (C, XC, YC, XYC):
            out_arrived(q, s).wait_recv()
        for s in range(1, 8):
            out_copy(q, s).wait_send()
    for k in range(CHUNKS):
        for s in range(1, 8):
            weight_copy(k, s).wait_send()
    for i in range(IMGS):
        image_copy(i).wait_send()
    for c in (vec_copy, hid_x, hid_c, hid_xc):
        c.wait_send()


def mega(x_in, wq, wk, wv, wo, wup, wdown, vec, hid):
    any_spec = pl.BlockSpec(memory_space=pl.ANY)
    vm = pl.BlockSpec(memory_space=pltpu.VMEM)
    dma = pltpu.SemaphoreType.DMA
    shapes = (x_in.shape, (LAYERS, 7, 4 * GF, HW), (LAYERS, 7, HW, FB), (LAYERS, 7, FB, HW))
    flops = 2 * 2048 * 1536 * 16384 * LAYERS
    return pl.pallas_call(
        mega_kernel,
        out_shape=tuple(jax.ShapeDtypeStruct(s, BF16) for s in shapes),
        in_specs=[any_spec] * 7 + [vm] * 2,
        out_specs=[any_spec] * 4,
        scratch_shapes=[
            pltpu.VMEM((IMGS, NTOK, HW), BF16), pltpu.VMEM((IMGS, NTOK, HW), BF16),
            pltpu.VMEM((IMGS * NTOK, 2 * HW), BF16), pltpu.VMEM((IMGS * NTOK, 4 * FB), BF16),
            pltpu.VMEM((2, 2 * HW, 4 * UC), BF16), pltpu.VMEM((2, 4 * FB, 2 * DC), BF16),
            pltpu.VMEM(vec.shape, F32), pltpu.VMEM((4,) + hid.shape, F32),
            dma((CHUNKS, 7)), dma((CHUNKS, 7)), dma((IMGS,)), dma((IMGS,)), dma((UNITS, 7)), dma((UNITS, 7)),
            dma((4,)), dma((4,)), dma((2,)), dma((8, 4)), dma((2, 8)), dma((3, UNITS)),
        ],
        compiler_params=pltpu.CompilerParams(collective_id=0, has_side_effects=True, vmem_limit_bytes=67043328),
        cost_estimate=pl.CostEstimate(flops=flops, bytes_accessed=300 << 20, transcendentals=0),
        name="encoder",
    )(x_in, wq, wk, wv, wo, wup, wdown, vec, hid)[0]


def solution(mesh):
    act_spec = P("dp", None, "tx")
    vec_tx = P(None, "tx")
    proj_spec = P(None, "tx", "ty", None)
    head_vec = P(None, "ty", None)
    in_specs = (act_spec, vec_tx, vec_tx, proj_spec, head_vec, proj_spec, proj_spec, head_vec,
                P(None, "ty", None, "tx"), vec_tx, vec_tx, vec_tx,
                P(None, "tx", "ty"), P(None, "ty"), P(None, "ty", "tx"), vec_tx)

    def heads_first(w):
        return jnp.transpose(w, (0, 2, 3, 1)).reshape(LAYERS, GF, HW)

    def local_fn(x_in, ln1_gain, ln1_bias, w_q, b_q, w_k, w_v, b_v, w_o, b_o, ln2_gain, ln2_bias, w_up, b_up, w_down, b_down):
        vec = jnp.stack([ln1_gain, ln1_bias, b_o, ln2_gain, ln2_bias, b_down], 1).reshape(6 * LAYERS, HW)
        vec = jnp.pad(vec, ((0, 16 - 6 * LAYERS), (0, 0)))
        hid = jnp.concatenate([b_q.reshape(LAYERS, GF), b_v.reshape(LAYERS, GF), b_up], -1)
        hid = jnp.pad(hid, ((0, 8 - LAYERS), (0, 0)))
        return mega(x_in, heads_first(w_q), heads_first(w_k), heads_first(w_v), w_o.reshape(LAYERS, GF, HW),
                    w_up, w_down, vec, hid)

    return jax.shard_map(local_fn, mesh=mesh, in_specs=in_specs, out_specs=act_spec, check_vma=False)
```

```python
import math

import jax
import jax.numpy as jnp
from jax import lax
from jax.experimental import pallas as pl
from jax.experimental.pallas import tpu as pltpu
from jax.sharding import PartitionSpec as P

EPS = 1e-6
F32 = jnp.float32
BF16 = jnp.bfloat16
MESH = pl.DeviceIdType.MESH

IMGS = 8
NTOK = 256
TOKENS = IMGS * NTOK
TILES = 4
TT = 512
HD = 96
GH = 4
GF = GH * HD
HW = 768
FB = 1536
UC = 384
DC = 128
NA, NU = 4, 4
ND = 6
DB = 2
PER_LAYER = NA + NU + ND
LAYERS = 2
CHUNKS = LAYERS * PER_LAYER
UNITS = ND * TILES
NB = 768
VR = HD + 16

X, Y, C = 2, 4, 1
XC, YC, XY, XYC = 3, 5, 6, 7

NN = (((1,), (0,)), ((), ()))
NT = (((1,), (1,)), ((), ()))
TN = (((0,), (0,)), ((), ()))


def dot(a, b, dims=NN):
    return lax.dot_general(a, b, dims, preferred_element_type=F32)


def gelu(x):
    return 0.5 * x * (1.0 + jnp.tanh(x * (0.7978845608028654 + 0.035677408136300125 * (x * x))))


def chunk_kind(k):
    layer, j = divmod(k, PER_LAYER)
    if j < NA:
        return layer, "a", j
    if j < NA + NU:
        return layer, "u", j - NA
    return layer, "d", j - NA - NU


LINK = 46.6e3
BACKLOG = 12.0
MODES = "xxxxxyxxyxxxyxxyyyyxyxyyyyyy"
RANK_X = "fhihkapyflvgprzumqtwuwsxzzzu"
RANK_Y = "hlbjoqorrtnphopfjmmonfkjiljh"
RANK_R = "cxtlosbypmfyjtepgfjseseimaah"
RANK_I = "coboceni"
EARLY, OUTS = 17, 2
BLOCKS = {"a": 16, "p": TILES, "u": NU * TILES, "d": ND * TILES}


def behind(letter):
    return 5 * (ord(letter) - ord("m"))


def relay_on_x(k):
    return MODES[k] == "x"


def chunk_bytes(k):
    return 2 * (FB * DC if chunk_kind(k)[1] == "d" else GF * HW)


def block_cost(kind, n):
    if kind == "a":
        return 3.06 + (1.25 if n < 4 else 0.0)
    return {"p": 3.87, "u": 3.16, "d": 46.0 / (ND * TILES)}[kind]


def plan():
    free = {"x": 0.0, "y": 0.0, "c": 0.0}
    ready = {}
    pending = []
    program = []
    now = [4.5]
    queue = {"x": [(10 * k + behind(RANK_X[k]), ("ownx", k)) for k in range(CHUNKS)],
             "y": [(10 * k + behind(RANK_Y[k]), ("owny", k)) for k in range(CHUNKS)]
             + [(20 + 3 * i + behind(RANK_I[i]), ("image", i)) for i in range(IMGS)]}
    given = set()
    passed = {None}
    unit = TT * DC * 2

    def send(link, size):
        rate, lag = (450e3, 1.5) if link == "c" else (LINK, 2.5)
        free[link] = max(free[link], now[0]) + size / rate
        return free[link] + lag

    def arrive(name, time, action=None):
        ready[name] = time
        if action is not None:
            pending.append((time, action))

    loads = []
    for layer in range(LAYERS):
        base = layer * PER_LAYER
        old = (layer - 1, "d", BLOCKS["d"] - 1) if layer else None
        for r in range(4):
            loads.append((("la", layer, r), [("w", s, base + j) for s in (r, 4 + r) if s for j in range(3)], old, 1.9))
        loads.append((("lo", layer), [("w", s, base + 3) for s in range(1, 8)], old, 2.2))
        for k in range(NU):
            last = (layer, "u", (k - 2) * TILES + TILES - 1) if k > 1 else old and (layer - 1, "u", BLOCKS["u"] - 1)
            loads.append((("lu", layer, k), [("w", s, base + NA + k) for s in range(1, 8)], last, 2.2))
        for j in range(ND):
            last = (layer, "d", (j - DB) * TILES + TILES - 1) if j >= DB else (layer, "p", TILES - 1)
            loads.append((("ld", layer, j), [("w", s, base + NA + NU + j) for s in range(1, 8)], last, 1.8))

    def do(action):
        program.append(("do", action))
        kind, *k = action
        k = k[0] if k else None
        if kind == "ownx":
            arrive(("w", X, k), send("x", chunk_bytes(k)), ("gotx", k))
        elif kind == "owny":
            arrive(("w", Y, k), send("y", chunk_bytes(k)), ("goty", k))
        elif kind == "ownc":
            arrive(("w", C, k), send("c", chunk_bytes(k)))
        elif kind == "image":
            arrive(("image", k), send("y", NTOK * HW * 2))
        elif kind == "gotx":
            arrive(("w", XC, k), send("c", chunk_bytes(k)))
            if not relay_on_x(k):
                queue["y"].append((10 * k + behind(RANK_R[k]), ("relay", k)))
        elif kind == "goty":
            arrive(("w", YC, k), send("c", chunk_bytes(k)))
            if relay_on_x(k):
                queue["x"].append((10 * k + behind(RANK_R[k]), ("relay", k)))
        elif kind == "relay":
            arrive(("w", XY, k), send("x" if relay_on_x(k) else "y", chunk_bytes(k)), ("gotd", k))
        elif kind == "gotd":
            arrive(("w", XYC, k), send("c", chunk_bytes(k)))
        elif kind == "out":
            queue["y"].append((10 * CHUNKS - EARLY + OUTS * k, ("outp", k)))
            arrive(("o", X, k), send("x", unit), ("outx", k))
            arrive(("o", C, k), send("c", unit))
        elif kind == "outp":
            arrive(("o", Y, k), send("y", unit), ("outy", k))
        elif kind == "outx":
            arrive(("o", XC, k), send("c", unit))
        elif kind == "outy":
            arrive(("o", XY, k), send("x", unit), ("outd", k))
            arrive(("o", YC, k), send("c", unit))
        elif kind == "outd":
            arrive(("o", XYC, k), send("c", unit))

    def pump():
        while True:
            due = [p for p in pending if p[0] <= now[0]]
            if due:
                first = min(due)
                pending.remove(first)
                do(first[1])
                continue
            for link in ("y", "x"):
                if queue[link] and free[link] - now[0] < BACKLOG:
                    first = min(queue[link])
                    queue[link].remove(first)
                    do(first[1])
                    if first[1][0] in ("ownx", "owny") and first[1][1] not in given:
                        given.add(first[1][1])
                        do(("ownc", first[1][1]))
                    break
            else:
                break
        for load in list(loads):
            action, needs, last, cost = load
            if last in passed and all(ready.get(a, 1e9) <= now[0] for a in needs):
                loads.remove(load)
                program.append(("do", action))
                ready[action] = now[0] + cost

    def block(layer, kind, n, needs, cost):
        while True:
            pump()
            late = [ready.get(a, 1e9) for a in needs if ready.get(a, 1e9) > now[0]]
            if not late:
                break
            times = [p[0] for p in pending] + [t for t in ready.values() if t > now[0]]
            times += [free[link] - BACKLOG + 1e-6 for link in queue if queue[link]]
            now[0] = max(now[0], min(times))
        program.append(("block", layer, kind, n))
        passed.add((layer, kind, n))
        now[0] += cost

    mark = []
    do(("small",))
    pump()
    for layer in range(LAYERS):
        for n in range(BLOCKS["a"]):
            needs = [("la", layer, n // 4)]
            if layer == 0 and n < 4:
                needs += [("image", 2 * n), ("image", 2 * n + 1)]
            block(layer, "a", n, needs, block_cost("a", n))
        for n in range(TILES):
            block(layer, "p", n, [("lo", layer)], block_cost("p", n))
        for n in range(BLOCKS["u"]):
            block(layer, "u", n, [("lu", layer, n // TILES)], block_cost("u", n))
        for n in range(BLOCKS["d"]):
            if layer == LAYERS - 1 and n == 0:
                do(("leave",))
            block(layer, "d", n, [("ld", layer, n // TILES)], block_cost("d", n))
            mark.append(now[0])
            if layer == LAYERS - 1 and n >= 1:
                do(("out", n - 1))
    do(("out", UNITS - 1))
    while pending or queue["y"]:
        times = [p[0] for p in pending] + [free["y"] - BACKLOG + 1e-6 for _ in queue["y"]]
        now[0] = max(now[0], min(times))
        pump()
    return program, max(now[0], max(ready.values())), mark


def mega_kernel(x_in, wq, wk, wv, wo, wup, wdown, *rest):
    vec_own, hid_own, rest = rest[:6], rest[6:9], rest[9:]
    big, land_a, land_u, land_d, x1, u, dbuf, qkv = rest[:8]
    vec_oth, hid, rest = rest[8:14], rest[14:17], rest[17:]
    encoder_body(x_in, wq, wk, wv, wo, wup, wdown, vec_own, hid_own, big, land_a, land_u, land_d,
                 x1, u, dbuf, qkv, vec_oth, hid, *rest)


def encoder_body(x_in, wq, wk, wv, wo, wup, wdown, vec_own, hid_own, big, land_a, land_u, land_d,
                 x1, u, dbuf, qkv, vec_oth, hid,
                wsend, wrecv, isend, irecv, osend, orecv, small_send, small_recv,
                local_sem, asem, usem, dsem, credit):
    ty, tx = lax.axis_index("ty"), lax.axis_index("tx")
    core, xx = lax.rem(ty, 2), ty // 2
    me = tx * 4 + ty
    x0 = big.at[0:TOKENS, 0:HW]
    h = big.at[TOKENS:2 * TOKENS, :]
    over_x = {"ty": (1 - xx) * 2 + core}
    over_y = {"tx": 1 - tx}
    over_c = {"ty": xx * 2 + (1 - core)}
    src_wa = (wq, wk, wv, wo)

    barrier = pltpu.get_barrier_semaphore()
    for peer in (over_x, over_y, over_c):
        pl.semaphore_signal(barrier, inc=1, device_id=peer, device_id_type=MESH)
    pl.semaphore_wait(barrier, 3)

    def remote(src, dst, send, recv, peer):
        return pltpu.make_async_remote_copy(src_ref=src, dst_ref=dst, send_sem=send, recv_sem=recv,
                                            device_id=peer, device_id_type=MESH)

    def own_ref(k):
        layer, kind, j = chunk_kind(k)
        if kind == "a":
            return src_wa[j].at[layer]
        if kind == "u":
            return wup.at[layer, :, j * UC:(j + 1) * UC]
        return wdown.at[layer, :, j * DC:(j + 1) * DC]

    def land_ref(k, s):
        layer, kind, j = chunk_kind(k)
        if kind == "a":
            return land_a.at[layer, s - 1, j * GF:(j + 1) * GF, :]
        if kind == "u":
            return land_u.at[layer, s - 1, :, j * UC:(j + 1) * UC]
        return land_d.at[layer, s - 1, :, j * DC:(j + 1) * DC]

    def weight_copy(k, s):
        if s == X:
            src, peer = own_ref(k), over_x
        elif s == Y:
            src, peer = own_ref(k), over_y
        elif s == C:
            src, peer = own_ref(k), over_c
        elif s == XY:
            src, peer = (land_ref(k, Y), over_x) if relay_on_x(k) else (land_ref(k, X), over_y)
        else:
            src, peer = land_ref(k, s - 1), over_c
        return remote(src, land_ref(k, s), wsend.at[k, s - 1], wrecv.at[k, s - 1], peer)

    def image_copy(i):
        theirs = (1 - tx) * 4 + ty
        return remote(x_in.at[theirs * IMGS + i], x1.at[i * NTOK:(i + 1) * NTOK, :], isend.at[i], irecv.at[i], over_y)

    def out_ref(s, q):
        cc, i = divmod(q, TILES)
        row, col = (s // 2) * TOKENS + i * TT, (s % 2) * HW + cc * DC
        return big.at[row:row + TT, col:col + DC]

    def out_copy(q, s):
        cc, i = divmod(q, TILES)
        if s == X:
            src, peer = out_ref(0, q), over_x
        elif s == C:
            src, peer = out_ref(0, q), over_c
        elif s == Y:
            src, peer = x1.at[i * TT:(i + 1) * TT, cc * DC:(cc + 1) * DC], over_y
        elif s == XY:
            src, peer = out_ref(Y, q), over_x
        else:
            src, peer = out_ref(s - 1, q), over_c
        return remote(src, out_ref(s, q), osend.at[q, s - 1], orecv.at[q, s - 1], peer)

    def out_arrived(q, s):
        return remote(out_ref(s, q), out_ref(s, q), osend.at[q, s - 1], orecv.at[q, s - 1], over_x)

    def small(src, dst, j, peer):
        return remote(src, dst, small_send.at[j], small_recv.at[j], peer)

    def vec_copy(j):
        return small(vec_own[j], vec_oth[j], j, over_y)

    def hid_copy(j, s):
        src = hid[j].at[X] if s == XC else hid_own[j]
        return small(src, hid[j].at[s], 6 + 3 * j + s - 1, over_x if s == X else over_c)

    def own_rows(i):
        return pltpu.make_async_copy(x_in.at[me * IMGS + i], big.at[i * NTOK:(i + 1) * NTOK, 0:HW], local_sem.at[i])

    def act(action):
        kind, *k = action
        k = k[0] if k else None
        if kind == "small":
            for j in range(3):
                hid_copy(j, X).start()
            for j in range(3):
                hid_copy(j, C).start()
            for j in range(6):
                vec_copy(j).start()
            for i in range(IMGS):
                own_rows(i).start()
        elif kind == "ownx":
            weight_copy(k, X).start()
        elif kind == "owny":
            weight_copy(k, Y).start()
        elif kind == "ownc":
            weight_copy(k, C).start()
        elif kind == "image":
            image_copy(k).start()
        elif kind == "gotx":
            weight_copy(k, X).wait_recv()
            weight_copy(k, XC).start()
        elif kind == "goty":
            weight_copy(k, Y).wait_recv()
            weight_copy(k, YC).start()
        elif kind == "relay":
            weight_copy(k, XY).start()
        elif kind == "gotd":
            weight_copy(k, XY).wait_recv()
            weight_copy(k, XYC).start()
        elif kind == "out":
            if k == 0:
                pl.semaphore_wait(credit, 3)
            for s in (X, C):
                out_copy(k, s).start()
        elif kind == "outp":
            out_copy(k, Y).start()
        elif kind == "leave":
            for peer in (over_x, over_y, over_c):
                pl.semaphore_signal(credit, inc=1, device_id=peer, device_id_type=MESH)
        elif kind == "outx":
            out_arrived(k, X).wait_recv()
            out_copy(k, XC).start()
        elif kind == "outy":
            out_arrived(k, Y).wait_recv()
            out_copy(k, XY).start()
            out_copy(k, YC).start()
        elif kind == "outd":
            out_arrived(k, XY).wait_recv()
            out_copy(k, XYC).start()
        elif kind == "la":
            layer, r = action[1:]
            for s in (r, 4 + r):
                if s % 2:
                    for j in range(3):
                        weight_copy(layer * PER_LAYER + j, s).wait_recv()
            start(a_loads(layer, r))
        elif kind == "lo":
            arrived(action[1] * PER_LAYER + 3)
            start(o_loads(action[1]))
        elif kind == "lu":
            arrived(action[1] * PER_LAYER + NA + action[2])
            start(u_loads(*action[1:]))
        elif kind == "ld":
            arrived(action[1] * PER_LAYER + NA + NU + action[2])
            start(d_loads(*action[1:]))

    def slot_ref(land, own, layer, s):
        return own.at[layer] if s == 0 else land.at[layer, s - 1]

    def a_loads(layer, r):
        out = []
        for dy in range(2):
            s = dy * 4 + r
            cols = slice(r * 2 * HW + dy * HW, r * 2 * HW + (dy + 1) * HW)
            if s == 0:
                for j in range(3):
                    out.append((src_wa[j].at[layer], u.at[j * GF:(j + 1) * GF, cols], asem.at[s, j]))
            else:
                out.append((land_a.at[layer, s - 1, 0:3 * GF, :], u.at[0:3 * GF, cols], asem.at[s, 0]))
        return [pltpu.make_async_copy(*c) for c in out]

    def o_loads(layer):
        out = []
        for r in range(4):
            for dy in range(2):
                s = dy * 4 + r
                src = wo.at[layer] if s == 0 else land_a.at[layer, s - 1, 3 * GF:4 * GF, :]
                at = 3 * GF + (r % 2) * GF
                cols = slice((r // 2) * 2 * HW + dy * HW, (r // 2) * 2 * HW + (dy + 1) * HW)
                out.append(pltpu.make_async_copy(src, u.at[at:at + GF, cols], asem.at[s, 3]))
        return out

    def u_loads(layer, k):
        b = k % 2
        out = []
        for r in range(4):
            for dy in range(2):
                s = dy * 4 + r
                src = slot_ref(land_u, wup, layer, s).at[:, k * UC:(k + 1) * UC]
                out.append(pltpu.make_async_copy(
                    src, big.at[(2 + b) * TOKENS + dy * HW:(2 + b) * TOKENS + (dy + 1) * HW, r * UC:(r + 1) * UC], usem.at[b, s]))
        return out

    def d_loads(layer, cc):
        b = cc % DB
        out = []
        for r in range(4):
            for dy in range(2):
                s = dy * 4 + r
                src = slot_ref(land_d, wdown, layer, s).at[:, cc * DC:(cc + 1) * DC]
                out.append(pltpu.make_async_copy(
                    src, dbuf.at[b, r * FB:(r + 1) * FB, dy * DC:(dy + 1) * DC], dsem.at[b, s]))
        return out

    def start(copies):
        for c in copies:
            c.start()

    def finish(copies):
        for c in copies:
            c.wait()

    def arrived(k):
        for s in (C, XC, YC, XYC):
            weight_copy(k, s).wait_recv()

    def vec_row(layer, j):
        return vec_own[j][layer:layer + 1, :], vec_oth[j][layer:layer + 1, :]

    def norm(layer, j, tile):
        g0, g1 = vec_row(layer, j)
        s0, s1 = vec_row(layer, j + 1)
        rows, group = 16, 8

        @pl.loop(0, TT // (rows * group))
        def _(i):
            ats = [pl.ds(pl.multiple_of(tile * TT + (i * group + m) * rows, rows), rows) for m in range(group)]
            pairs = [(x0[at, :].astype(F32), x1[at, :].astype(F32)) for at in ats]
            done = []
            for a, b in pairs:
                mean = jnp.sum(a + b, 1, keepdims=True) * (0.5 / HW)
                a = a - mean
                b = b - mean
                var = jnp.sum(a * a + b * b, 1, keepdims=True) * (0.5 / HW)
                inv = lax.rsqrt(var + EPS)
                done.append(((a * inv * g0 + s0).astype(BF16), (b * inv * g1 + s1).astype(BF16)))
            for at, (a, b) in zip(ats, done):
                h[at, :HW] = a
                h[at, HW:] = b

    scale = HD ** -0.5 * math.log2(math.e)

    def qkv_at(b, first, rows):
        return qkv.at[first:first + rows, :]

    def ones_rows():
        for hd in range(GH):
            qkv_at(0, 2 * GF + hd * VR + HD, 16)[...] = jnp.ones((16, TT), BF16)

    def column(ref, layer, r):
        rows = [jnp.broadcast_to(ref[r, layer, hd:hd + 1, :], (128, HD)).T for hd in range(GH)]
        col = jnp.concatenate(rows, 0)
        return jnp.concatenate([col] * (TT // 128), 1)

    def project_qkv(layer, n):
        r, tile, b = n // 4, lax.rem(n, 4), 0
        rows = pl.ds(pl.multiple_of(tile * TT, TT), TT)
        cols = pl.ds(pl.multiple_of(r * 2 * HW, 2 * HW), 2 * HW)
        t = dot(u[0:3 * GF, cols], h[rows, :], NT)
        qkv_at(b, 0, GF)[...] = (t[:GF] + column(hid[0], layer, r)).astype(BF16)
        qkv_at(b, GF, GF)[...] = t[GF:2 * GF].astype(BF16)
        t = (t[2 * GF:] + column(hid[1], layer, r)).astype(BF16)
        for hd in range(GH):
            qkv_at(b, 2 * GF + hd * VR, HD)[...] = t[hd * HD:(hd + 1) * HD, :]

    def heads(n):
        r, tile, b = n // 4, lax.rem(n, 4), 0
        score, weigh, value = [], [], []
        for img in range(TT // NTOK):
            c = slice(img * NTOK, (img + 1) * NTOK)
            for hd in range(GH):
                box = {}

                def f(hd=hd, c=c, box=box):
                    qt = qkv_at(b, hd * HD, HD)[:, c]
                    kt = qkv_at(b, GF + hd * HD, HD)[:, c]
                    box["s"] = dot(kt, qt, TN)

                def g(box=box):
                    st = box["s"]
                    box["e"] = jnp.exp2((st - jnp.max(st, 0, keepdims=True)) * scale).astype(BF16)

                def w(hd=hd, c=c, img=img, box=box):
                    t = dot(qkv_at(b, 2 * GF + hd * VR, VR)[:, c], box["e"])
                    at = pl.ds(pl.multiple_of(tile * 4 * GF + r * GF + hd * HD, 16), HD)
                    dbuf[img, at, :] = (t[:HD] * (1.0 / t[HD:HD + 1])).astype(BF16)
                score.append(f)
                weigh.append(g)
                value.append(w)
        return score, weigh, value

    def run_heads(n):
        score, weigh, value = heads(n)
        for f in score:
            f()
        for g, w in zip(weigh, value):
            g()
            w()

    def project_block(layer, tile):
        b0, b1 = vec_row(layer, 2)
        at = pl.ds(pl.multiple_of(tile * 4 * GF, 4 * GF), 4 * GF)
        o = jnp.concatenate([dbuf[img, at, :].T for img in range(TT // NTOK)], 0)
        rows = pl.ds(pl.multiple_of(tile * TT, TT), TT)
        for half, ref, bias in ((0, x0, b0), (1, x1, b1)):
            acc = dot(o[:, :HW], u[3 * GF:5 * GF, half * HW:(half + 1) * HW])
            acc += dot(o[:, HW:], u[3 * GF:5 * GF, 2 * HW + half * HW:2 * HW + (half + 1) * HW])
            ref[rows, :] = (ref[rows, :].astype(F32) + acc + bias).astype(BF16)

    def up_block(layer, k, tile, b):
        rows = pl.ds(pl.multiple_of(tile * TT, TT), TT)
        bias = jnp.concatenate(
            [hid[2][r, layer:layer + 1, pl.ds(pl.multiple_of(k * UC, 128), UC)] for r in range(4)], 1)
        for first in range(0, 4 * UC, NB):
            t = gelu(dot(h[rows, :], big[pl.ds(pl.multiple_of((2 + b) * TOKENS, TOKENS), 2 * HW), first:first + NB]) + bias[:, first:first + NB]).astype(BF16)
            at = first
            while at < first + NB:
                r, off = divmod(at, UC)
                size = min(UC - off, first + NB - at)
                u[rows, pl.ds(pl.multiple_of(r * FB + k * UC + off, 128), size)] = t[:, at - first:at - first + size]
                at += size

    def down_block(layer, cc, tile, b):
        rows = pl.ds(pl.multiple_of(tile * TT, TT), TT)
        cols = pl.ds(pl.multiple_of(cc * DC, DC), DC)
        acc = dot(u[rows, :], dbuf[b])
        for half, ref, vec in ((0, x0, vec_own[5]), (1, x1, vec_oth[5])):
            new = ref[rows, cols].astype(F32) + acc[:, half * DC:(half + 1) * DC] + vec[layer:layer + 1, cols]
            ref[rows, cols] = new.astype(BF16)

    program, _, _ = plan()
    before = {}
    todo = []
    tail = []
    for item in program:
        if item[0] == "do":
            todo.append(item[1])
        else:
            before[item[1:]] = todo
            todo = []
    tail = todo

    def ahead(layer, kind, n, first=0):
        def branch(some):
            if len(some) == 1:
                for a in before[(layer, kind, some[0])] if some[0] >= first else ():
                    act(a)
                return
            half = len(some) // 2

            @pl.when(n < some[half])
            def _():
                branch(some[:half])

            @pl.when(n >= some[half])
            def _():
                branch(some[half:])

        branch(range(BLOCKS[kind]))

    def straight(layer, kind, n):
        for a in before[(layer, kind, n)]:
            act(a)

    def at_loads(n, count, wait):
        for j in range(count):
            @pl.when(n == j * TILES)
            def _(j=j):
                finish(wait(j))

    def norm_first(layer, tile):
        if layer == 0:
            for i in range(2):
                image_copy(2 * tile + i).wait_recv()
        norm(layer, 0, tile)

    for layer in range(LAYERS):
        straight(layer, "a", 0)
        if layer == 0:
            for j in range(3):
                hid_copy(j, X).wait_recv()
                hid_copy(j, XC).start()
            for j in range(3):
                hid_copy(j, C).wait_recv()
                hid_copy(j, XC).wait_recv()
                hid[j][0] = hid_own[j][...]
            for j in range(6):
                vec_copy(j).wait_recv()
            for i in range(IMGS):
                own_rows(i).wait()
        ones_rows()

        @pl.loop(0, 4 * TILES)
        def _(n, layer=layer):
            ahead(layer, "a", n, 1)
            for r in range(4):
                @pl.when(n == 4 * r)
                def _(r=r):
                    finish(a_loads(layer, r))
            for tile in range(TILES):
                @pl.when(n == tile)
                def _(tile=tile):
                    norm_first(layer, tile)
            project_qkv(layer, n)

            @pl.when(n < BLOCKS["a"])
            def _():
                run_heads(n)

        @pl.loop(0, TILES)
        def _(n, layer=layer):
            ahead(layer, "p", n)

            @pl.when(n == 0)
            def _():
                finish(o_loads(layer))
            project_block(layer, n)
            norm(layer, 3, n)

        @pl.loop(0, NU * TILES)
        def _(n, layer=layer):
            ahead(layer, "u", n)
            k, tile = n // TILES, lax.rem(n, TILES)
            at_loads(n, NU, lambda j: u_loads(layer, j))
            up_block(layer, k, tile, lax.rem(k, 2))

        @pl.loop(0, ND * TILES)
        def _(n, layer=layer):
            ahead(layer, "d", n)
            cc, tile = n // TILES, lax.rem(n, TILES)
            at_loads(n, ND, lambda j: d_loads(layer, j))
            down_block(layer, cc, tile, lax.rem(cc, DB))

    for k in range(CHUNKS):
        for s in range(1, 8):
            weight_copy(k, s).wait_send()
    for i in range(IMGS):
        image_copy(i).wait_send()
    for j in range(6):
        vec_copy(j).wait_send()
    for j in range(3):
        for s in (X, C, XC):
            hid_copy(j, s).wait_send()
    def close(q):
        for s in (C, XC, YC, XYC):
            out_arrived(q, s).wait_recv()
        for s in range(1, 8):
            out_copy(q, s).wait_send()

    closed = 0
    for a in tail:
        act(a)
        if a[0] == "outd":
            while closed < a[1] - 3:
                close(closed)
                closed += 1
    for q in range(closed, UNITS):
        close(q)


def mega(x_in, wq, wk, wv, wo, wup, wdown, *small):
    any_spec = pl.BlockSpec(memory_space=pl.ANY)
    vm = pl.BlockSpec(memory_space=pltpu.VMEM)
    dma = pltpu.SemaphoreType.DMA
    shapes = ((LAYERS, 7, 4 * GF, HW), (LAYERS, 7, HW, FB), (LAYERS, 7, FB, HW))
    flops = 2 * TOKENS * FB * 16384 * LAYERS
    return pl.pallas_call(
        mega_kernel,
        out_shape=(pltpu.VMEM((4 * TOKENS, 2 * HW), BF16),) + tuple(jax.ShapeDtypeStruct(s, BF16) for s in shapes),
        in_specs=[any_spec] * 7 + [vm] * 9,
        out_specs=[vm] + [any_spec] * 3,
        scratch_shapes=[
            pltpu.VMEM((TOKENS, HW), BF16), pltpu.VMEM((TOKENS, 4 * FB), BF16),
            pltpu.VMEM((DB, 4 * FB, 2 * DC), BF16), pltpu.VMEM((2 * GF + GH * VR, TT), BF16),
            *[pltpu.VMEM(a.shape, F32) for a in small[:6]], *[pltpu.VMEM((4,) + a.shape, F32) for a in small[6:]],
            dma((CHUNKS, 7)), dma((CHUNKS, 7)), dma((IMGS,)), dma((IMGS,)), dma((UNITS, 7)), dma((UNITS, 7)),
            dma((15,)), dma((15,)), dma((IMGS,)), dma((8, 4)), dma((2, 8)), dma((DB, 8)), pltpu.SemaphoreType.REGULAR,
        ],
        compiler_params=pltpu.CompilerParams(collective_id=0, has_side_effects=True, vmem_limit_bytes=41000000),
        cost_estimate=pl.CostEstimate(flops=flops, bytes_accessed=300 << 20, transcendentals=0),
        name="encoder",
    )(x_in, wq, wk, wv, wo, wup, wdown, *small)[0]


def hand_over(big, shape):
    def copy(big_ref, out_ref, sems):
        me = lax.axis_index("tx") * 4 + lax.axis_index("ty")
        copies = []
        for s in range(8):
            place = sum(((me // bit + s // bit) % 2) * bit for bit in (1, 2, 4))
            for i in range(IMGS):
                row, col = (s // 2) * TOKENS + i * NTOK, (s % 2) * HW
                copies.append(pltpu.make_async_copy(
                    big_ref.at[row:row + NTOK, col:col + HW], out_ref.at[place * IMGS + i], sems.at[s, i]))
        for c in copies:
            c.start()
        for c in copies:
            c.wait()

    return pl.pallas_call(
        copy, out_shape=jax.ShapeDtypeStruct(shape, big.dtype),
        in_specs=[pl.BlockSpec(memory_space=pltpu.VMEM)], out_specs=pl.BlockSpec(memory_space=pl.ANY),
        scratch_shapes=[pltpu.SemaphoreType.DMA((8, IMGS))],
        compiler_params=pltpu.CompilerParams(vmem_limit_bytes=1 << 20), name="hand_over")(big)


def solution(mesh):
    act_spec = P("dp", None, "tx")
    vec_tx = P(None, "tx")
    proj_spec = P(None, "tx", "ty", None)
    head_vec = P(None, "ty", None)
    in_specs = (act_spec, vec_tx, vec_tx, proj_spec, head_vec, proj_spec, proj_spec, head_vec,
                P(None, "ty", None, "tx"), vec_tx, vec_tx, vec_tx,
                P(None, "tx", "ty"), P(None, "ty"), P(None, "ty", "tx"), vec_tx)

    def heads_first(w):
        return jnp.transpose(w, (0, 2, 3, 1)).reshape(LAYERS, GF, HW)

    def local_fn(x_in, ln1_gain, ln1_bias, w_q, b_q, w_k, w_v, b_v, w_o, b_o, ln2_gain, ln2_bias, w_up, b_up, w_down, b_down):
        big = mega(x_in, heads_first(w_q), heads_first(w_k), heads_first(w_v), w_o.reshape(LAYERS, GF, HW), w_up, w_down,
                   ln1_gain, ln1_bias, b_o, ln2_gain, ln2_bias, b_down, b_q, b_v, b_up)
        return hand_over(big, x_in.shape)

    return jax.shard_map(local_fn, mesh=mesh, in_specs=in_specs, out_specs=act_spec, check_vma=False)
```

```python
import math

import jax
import jax.numpy as jnp
from jax import lax
from jax.experimental import pallas as pl
from jax.experimental.pallas import tpu as pltpu
from jax.sharding import PartitionSpec as P

EPS = 1e-6
F32 = jnp.float32
BF16 = jnp.bfloat16
MESH = pl.DeviceIdType.MESH

IMGS = 8
NTOK = 256
TOKENS = IMGS * NTOK
TILES = 4
TT = 512
HD = 96
GH = 4
GF = GH * HD
HW = 768
FB = 1536
UC = 384
DC = 128
NA, NU = 4, 4
ND = 6
DB = 2
PER_LAYER = NA + NU + ND
LAYERS = 2
CHUNKS = LAYERS * PER_LAYER
UNITS = ND * TILES
NB = 768
VR = HD + 16

X, Y, C = 2, 4, 1
XC, YC, XY, XYC = 3, 5, 6, 7

NN = (((1,), (0,)), ((), ()))
NT = (((1,), (1,)), ((), ()))
TN = (((0,), (0,)), ((), ()))


def dot(a, b, dims=NN):
    return lax.dot_general(a, b, dims, preferred_element_type=F32)


def gelu(x):
    return 0.5 * x * (1.0 + jnp.tanh(x * (0.7978845608028654 + 0.035677408136300125 * (x * x))))


def chunk_kind(k):
    layer, j = divmod(k, PER_LAYER)
    if j < NA:
        return layer, "a", j
    if j < NA + NU:
        return layer, "u", j - NA
    return layer, "d", j - NA - NU


LINK = 46.6e3
BACKLOG = 12.0
MODES = "xxyxxxxxxyyxxxxyyyxyyxyyyyyy"
RANK_X = "qqqqddddiiiiiiccccnnnnjjjjjj"
RANK_Y = "ttttssssllllllqqqqssssqqqqqq"
RANK_R = "qqqqrrrraaaaaammmmffffrrrrrr"
RANK_I = "wjlqemul"
EARLY, OUTS = -20, 2
BLOCKS = {"a": 16, "p": TILES, "u": NU * TILES, "d": ND * TILES}


def behind(letter):
    return 5 * (ord(letter) - ord("m"))


def relay_on_x(k):
    return MODES[k] == "x"


def chunk_bytes(k):
    return 2 * (FB * DC if chunk_kind(k)[1] == "d" else GF * HW)


def block_cost(kind, n):
    if kind == "a":
        return 3.06 + (1.25 if n < 4 else 0.0)
    return {"p": 3.87, "u": 3.16, "d": 46.0 / (ND * TILES)}[kind]


def plan():
    free = {"x": 0.0, "y": 0.0, "c": 0.0}
    ready = {}
    pending = []
    program = []
    now = [4.5]
    queue = {"x": [(10 * k + behind(RANK_X[k]), ("ownx", k)) for k in range(CHUNKS)],
             "y": [(10 * k + behind(RANK_Y[k]), ("owny", k)) for k in range(CHUNKS)]
             + [(20 + 3 * i + behind(RANK_I[i]), ("image", i)) for i in range(IMGS)]}
    given = set()
    passed = {None}
    unit = TT * DC * 2

    def send(link, size):
        rate, lag = (450e3, 1.5) if link == "c" else (LINK, 2.5)
        free[link] = max(free[link], now[0]) + size / rate
        return free[link] + lag

    def arrive(name, time, action=None):
        ready[name] = time
        if action is not None:
            pending.append((time, action))

    loads = []
    for layer in range(LAYERS):
        base = layer * PER_LAYER
        old = (layer - 1, "d", BLOCKS["d"] - 1) if layer else None
        for r in range(4):
            loads.append((("la", layer, r), [("w", s, base + j) for s in (r, 4 + r) if s for j in range(3)], old, 1.9))
        loads.append((("lo", layer), [("w", s, base + 3) for s in range(1, 8)], old, 2.2))
        for k in range(NU):
            last = (layer, "u", (k - 2) * TILES + TILES - 1) if k > 1 else old and (layer - 1, "u", BLOCKS["u"] - 1)
            loads.append((("lu", layer, k), [("w", s, base + NA + k) for s in range(1, 8)], last, 2.2))
        for j in range(ND):
            last = (layer, "d", (j - DB) * TILES + TILES - 1) if j >= DB else (layer, "p", TILES - 1)
            loads.append((("ld", layer, j), [("w", s, base + NA + NU + j) for s in range(1, 8)], last, 1.8))

    def do(action):
        program.append(("do", action))
        kind, *k = action
        k = k[0] if k else None
        if kind == "ownx":
            arrive(("w", X, k), send("x", chunk_bytes(k)), ("gotx", k))
        elif kind == "owny":
            arrive(("w", Y, k), send("y", chunk_bytes(k)), ("goty", k))
        elif kind == "ownc":
            arrive(("w", C, k), send("c", chunk_bytes(k)))
        elif kind == "image":
            arrive(("image", k), send("y", NTOK * HW * 2))
        elif kind == "gotx":
            arrive(("w", XC, k), send("c", chunk_bytes(k)))
            if not relay_on_x(k):
                queue["y"].append((10 * k + behind(RANK_R[k]), ("relay", k)))
        elif kind == "goty":
            arrive(("w", YC, k), send("c", chunk_bytes(k)))
            if relay_on_x(k):
                queue["x"].append((10 * k + behind(RANK_R[k]), ("relay", k)))
        elif kind == "relay":
            arrive(("w", XY, k), send("x" if relay_on_x(k) else "y", chunk_bytes(k)), ("gotd", k))
        elif kind == "gotd":
            arrive(("w", XYC, k), send("c", chunk_bytes(k)))
        elif kind == "out":
            queue["y"].append((10 * CHUNKS - EARLY + OUTS * k, ("outp", k)))
            arrive(("o", X, k), send("x", unit), ("outx", k))
            arrive(("o", C, k), send("c", unit))
        elif kind == "outp":
            arrive(("o", Y, k), send("y", unit), ("outy", k))
        elif kind == "outx":
            arrive(("o", XC, k), send("c", unit))
        elif kind == "outy":
            arrive(("o", XY, k), send("x", unit), ("outd", k))
            arrive(("o", YC, k), send("c", unit))
        elif kind == "outd":
            arrive(("o", XYC, k), send("c", unit))

    def pump():
        while True:
            due = [p for p in pending if p[0] <= now[0]]
            if due:
                first = min(due)
                pending.remove(first)
                do(first[1])
                continue
            for link in ("y", "x"):
                if queue[link] and free[link] - now[0] < BACKLOG:
                    first = min(queue[link])
                    queue[link].remove(first)
                    do(first[1])
                    if first[1][0] in ("ownx", "owny") and first[1][1] not in given:
                        given.add(first[1][1])
                        do(("ownc", first[1][1]))
                    break
            else:
                break
        for load in list(loads):
            action, needs, last, cost = load
            if last in passed and all(ready.get(a, 1e9) <= now[0] for a in needs):
                loads.remove(load)
                program.append(("do", action))
                ready[action] = now[0] + cost

    def block(layer, kind, n, needs, cost):
        while True:
            pump()
            late = [ready.get(a, 1e9) for a in needs if ready.get(a, 1e9) > now[0]]
            if not late:
                break
            times = [p[0] for p in pending] + [t for t in ready.values() if t > now[0]]
            times += [free[link] - BACKLOG + 1e-6 for link in queue if queue[link]]
            now[0] = max(now[0], min(times))
        program.append(("block", layer, kind, n))
        passed.add((layer, kind, n))
        now[0] += cost

    mark = []
    do(("small",))
    pump()
    for layer in range(LAYERS):
        for n in range(BLOCKS["a"]):
            needs = [("la", layer, n // 4)]
            if layer == 0 and n < 4:
                needs += [("image", 2 * n), ("image", 2 * n + 1)]
            block(layer, "a", n, needs, block_cost("a", n))
        for n in range(TILES):
            block(layer, "p", n, [("lo", layer)], block_cost("p", n))
        for n in range(BLOCKS["u"]):
            block(layer, "u", n, [("lu", layer, n // TILES)], block_cost("u", n))
        for n in range(BLOCKS["d"]):
            if layer == LAYERS - 1 and n == 0:
                do(("leave",))
            block(layer, "d", n, [("ld", layer, n // TILES)], block_cost("d", n))
            mark.append(now[0])
            if layer == LAYERS - 1:
                do(("out", n))
    while pending or queue["y"]:
        times = [p[0] for p in pending] + [free["y"] - BACKLOG + 1e-6 for _ in queue["y"]]
        now[0] = max(now[0], min(times))
        pump()
    return program, max(now[0], max(ready.values())), mark


def mega_kernel(x_in, wq, wk, wv, wo, wup, wdown, *rest):
    vec_own, hid_own, rest = rest[:6], rest[6:9], rest[9:]
    big, land_a, land_u, land_d, x1, u, dbuf, qkv = rest[:8]
    vec_oth, hid, rest = rest[8:14], rest[14:17], rest[17:]
    encoder_body(x_in, wq, wk, wv, wo, wup, wdown, vec_own, hid_own, big, land_a, land_u, land_d,
                 x1, u, dbuf, qkv, vec_oth, hid, *rest)


def encoder_body(x_in, wq, wk, wv, wo, wup, wdown, vec_own, hid_own, big, land_a, land_u, land_d,
                 x1, u, dbuf, qkv, vec_oth, hid,
                wsend, wrecv, arecv, crecv, isend, irecv, osend, orecv, small_send, small_recv,
                local_sem, asem, usem, dsem, credit):
    ty, tx = lax.axis_index("ty"), lax.axis_index("tx")
    core, xx = lax.rem(ty, 2), ty // 2
    me = tx * 4 + ty
    x0 = big.at[0:TOKENS, 0:HW]
    h = big.at[TOKENS:2 * TOKENS, :]
    over_x = {"ty": (1 - xx) * 2 + core}
    over_y = {"tx": 1 - tx}
    over_c = {"ty": xx * 2 + (1 - core)}
    src_wa = (wq, wk, wv, wo)

    barrier = pltpu.get_barrier_semaphore()
    for peer in (over_x, over_y, over_c):
        pl.semaphore_signal(barrier, inc=1, device_id=peer, device_id_type=MESH)
    pl.semaphore_wait(barrier, 3)

    def remote(src, dst, send, recv, peer):
        return pltpu.make_async_remote_copy(src_ref=src, dst_ref=dst, send_sem=send, recv_sem=recv,
                                            device_id=peer, device_id_type=MESH)

    def own_ref(k):
        layer, kind, j = chunk_kind(k)
        if kind == "a":
            return src_wa[j].at[layer]
        if kind == "u":
            return wup.at[layer, :, j * UC:(j + 1) * UC]
        return wdown.at[layer, :, j * DC:(j + 1) * DC]

    def land_ref(k, s):
        layer, kind, j = chunk_kind(k)
        if kind == "a":
            return land_a.at[layer, s - 1, j * GF:(j + 1) * GF, :]
        if kind == "u":
            return land_u.at[layer, s - 1, :, j * UC:(j + 1) * UC]
        return land_d.at[layer, s - 1, :, j * DC:(j + 1) * DC]

    def weight_copy(k, s):
        if s == X:
            src, peer = own_ref(k), over_x
        elif s == Y:
            src, peer = own_ref(k), over_y
        elif s == C:
            src, peer = own_ref(k), over_c
        elif s == XY:
            src, peer = (land_ref(k, Y), over_x) if relay_on_x(k) else (land_ref(k, X), over_y)
        else:
            src, peer = land_ref(k, s - 1), over_c
        return remote(src, land_ref(k, s), wsend.at[s - 1], landed(k, s), peer)

    def landed(k, s):
        layer, kind, j = chunk_kind(k)
        hop = (X, Y, XY).index(s) if s in (X, Y, XY) else 3
        if kind != "a":
            return wrecv.at[k - (layer + 1) * NA, hop]
        if hop < 3:
            return arecv.at[layer * NA + j, hop]
        return crecv.at[layer, 4 if j == 3 else s // 2]

    def whole(ref, sem):
        return remote(ref, ref, wsend.at[0], sem, over_c).wait_recv()

    def image_copy(i):
        theirs = (1 - tx) * 4 + ty
        return remote(x_in.at[theirs * IMGS + i], x1.at[i * NTOK:(i + 1) * NTOK, :], isend.at[0], irecv.at[i // 2], over_y)

    def out_ref(s, q):
        cc, i = divmod(q, TILES)
        row, col = (s // 2) * TOKENS + i * TT, (s % 2) * HW + cc * DC
        return big.at[row:row + TT, col:col + DC]

    def out_copy(q, s):
        cc, i = divmod(q, TILES)
        if s == X:
            src, peer = out_ref(0, q), over_x
        elif s == C:
            src, peer = out_ref(0, q), over_c
        elif s == Y:
            src, peer = x1.at[i * TT:(i + 1) * TT, cc * DC:(cc + 1) * DC], over_y
        elif s == XY:
            src, peer = out_ref(Y, q), over_x
        else:
            src, peer = out_ref(s - 1, q), over_c
        return remote(src, out_ref(s, q), osend.at[s - 1], left(q, s), peer)

    def left(q, s):
        return orecv.at[q, (X, Y, XY).index(s)] if s in (X, Y, XY) else osend.at[7]

    def out_arrived(q, s):
        return remote(out_ref(s, q), out_ref(s, q), osend.at[s - 1], left(q, s), over_x)

    def small(src, dst, j, peer):
        return remote(src, dst, small_send.at[j], small_recv.at[j], peer)

    def vec_copy(j):
        return small(vec_own[j], vec_oth[j], j, over_y)

    def hid_copy(j, s):
        src = hid[j].at[X] if s == XC else hid_own[j]
        return small(src, hid[j].at[s], 6 + 3 * j + s - 1, over_x if s == X else over_c)

    def own_rows(i):
        return pltpu.make_async_copy(x_in.at[me * IMGS + i], big.at[i * NTOK:(i + 1) * NTOK, 0:HW], local_sem.at[0])

    def act(action):
        kind, *k = action
        k = k[0] if k else None
        if kind == "small":
            for j in range(3):
                hid_copy(j, X).start()
            for j in range(3):
                hid_copy(j, C).start()
            for j in range(6):
                vec_copy(j).start()
            for i in range(IMGS):
                own_rows(i).start()
        elif kind == "ownx":
            weight_copy(k, X).start()
        elif kind == "owny":
            weight_copy(k, Y).start()
        elif kind == "ownc":
            weight_copy(k, C).start()
        elif kind == "image":
            image_copy(k).start()
        elif kind == "gotx":
            weight_copy(k, X).wait_recv()
            weight_copy(k, XC).start()
        elif kind == "goty":
            weight_copy(k, Y).wait_recv()
            weight_copy(k, YC).start()
        elif kind == "relay":
            weight_copy(k, XY).start()
        elif kind == "gotd":
            weight_copy(k, XY).wait_recv()
            weight_copy(k, XYC).start()
        elif kind == "out":
            if k == 0:
                pl.semaphore_wait(credit, 3)
            for s in (X, C):
                out_copy(k, s).start()
        elif kind == "outp":
            out_copy(k, Y).start()
        elif kind == "leave":
            for peer in (over_x, over_y, over_c):
                pl.semaphore_signal(credit, inc=1, device_id=peer, device_id_type=MESH)
        elif kind == "outx":
            out_arrived(k, X).wait_recv()
            out_copy(k, XC).start()
        elif kind == "outy":
            out_arrived(k, Y).wait_recv()
            out_copy(k, XY).start()
            out_copy(k, YC).start()
        elif kind == "outd":
            out_arrived(k, XY).wait_recv()
            out_copy(k, XYC).start()
        elif kind == "la":
            layer, r = action[1:]
            for s in (r, 4 + r):
                if s % 2:
                    whole(land_a.at[layer, s - 1, 0:3 * GF, :], crecv.at[layer, s // 2])
            start(a_loads(layer, r))
        elif kind == "lo":
            arrived(action[1] * PER_LAYER + 3)
            start(o_loads(action[1]))
        elif kind == "lu":
            arrived(action[1] * PER_LAYER + NA + action[2])
            start(u_loads(*action[1:]))
        elif kind == "ld":
            arrived(action[1] * PER_LAYER + NA + NU + action[2])
            start(d_loads(*action[1:]))

    def slot_ref(land, own, layer, s):
        return own.at[layer] if s == 0 else land.at[layer, s - 1]

    def a_loads(layer, r):
        out = []
        for dy in range(2):
            s = dy * 4 + r
            cols = slice(r * 2 * HW + dy * HW, r * 2 * HW + (dy + 1) * HW)
            if s == 0:
                for j in range(3):
                    out.append((src_wa[j].at[layer], u.at[j * GF:(j + 1) * GF, cols], asem.at[r]))
            else:
                out.append((land_a.at[layer, s - 1, 0:3 * GF, :], u.at[0:3 * GF, cols], asem.at[r]))
        return [pltpu.make_async_copy(*c) for c in out]

    def o_loads(layer):
        out = []
        for r in range(4):
            for dy in range(2):
                s = dy * 4 + r
                src = wo.at[layer] if s == 0 else land_a.at[layer, s - 1, 3 * GF:4 * GF, :]
                at = 3 * GF + (r % 2) * GF
                cols = slice((r // 2) * 2 * HW + dy * HW, (r // 2) * 2 * HW + (dy + 1) * HW)
                out.append(pltpu.make_async_copy(src, u.at[at:at + GF, cols], asem.at[4]))
        return out

    def u_loads(layer, k):
        b = k % 2
        out = []
        for r in range(4):
            for dy in range(2):
                s = dy * 4 + r
                src = slot_ref(land_u, wup, layer, s).at[:, k * UC:(k + 1) * UC]
                out.append(pltpu.make_async_copy(
                    src, big.at[(2 + b) * TOKENS + dy * HW:(2 + b) * TOKENS + (dy + 1) * HW, r * UC:(r + 1) * UC], usem.at[b]))
        return out

    def d_loads(layer, cc):
        b = cc % DB
        out = []
        for r in range(4):
            for dy in range(2):
                s = dy * 4 + r
                src = slot_ref(land_d, wdown, layer, s).at[:, cc * DC:(cc + 1) * DC]
                out.append(pltpu.make_async_copy(
                    src, dbuf.at[b, r * FB:(r + 1) * FB, dy * DC:(dy + 1) * DC], dsem.at[b]))
        return out

    def start(copies):
        for c in copies:
            c.start()

    def loaded(ref, sem):
        pltpu.make_async_copy(ref, ref, sem).wait()

    def a_loaded(r):
        loaded(u.at[0:3 * GF, r * 2 * HW:(r + 1) * 2 * HW], asem.at[r])

    def o_loaded():
        loaded(u.at[3 * GF:5 * GF, 0:4 * HW], asem.at[4])

    def u_loaded(k):
        at = (2 + k % 2) * TOKENS
        loaded(big.at[at:at + 2 * HW, :], usem.at[k % 2])

    def d_loaded(cc):
        loaded(dbuf.at[cc % DB], dsem.at[cc % DB])

    def arrived(k):
        layer, kind, j = chunk_kind(k)
        if kind == "a":
            ref = land_a.at[layer, 0:4, j * GF:(j + 1) * GF, :]
        elif kind == "u":
            ref = land_u.at[layer, 0:4, :, j * UC:(j + 1) * UC]
        else:
            ref = land_d.at[layer, 0:4, :, j * DC:(j + 1) * DC]
        whole(ref, landed(k, C))

    def vec_row(layer, j):
        return vec_own[j][layer:layer + 1, :], vec_oth[j][layer:layer + 1, :]

    def norm(layer, j, tile):
        g0, g1 = vec_row(layer, j)
        s0, s1 = vec_row(layer, j + 1)
        rows, group = 16, 8

        @pl.loop(0, TT // (rows * group))
        def _(i):
            ats = [pl.ds(pl.multiple_of(tile * TT + (i * group + m) * rows, rows), rows) for m in range(group)]
            pairs = [(x0[at, :].astype(F32), x1[at, :].astype(F32)) for at in ats]
            done = []
            for a, b in pairs:
                mean = jnp.sum(a + b, 1, keepdims=True) * (0.5 / HW)
                a = a - mean
                b = b - mean
                var = jnp.sum(a * a + b * b, 1, keepdims=True) * (0.5 / HW)
                inv = lax.rsqrt(var + EPS)
                done.append(((a * inv * g0 + s0).astype(BF16), (b * inv * g1 + s1).astype(BF16)))
            for at, (a, b) in zip(ats, done):
                h[at, :HW] = a
                h[at, HW:] = b

    scale = HD ** -0.5 * math.log2(math.e)

    def qkv_at(b, first, rows):
        return qkv.at[first:first + rows, :]

    def ones_rows():
        for hd in range(GH):
            qkv_at(0, 2 * GF + hd * VR + HD, 16)[...] = jnp.ones((16, TT), BF16)

    def column(ref, layer, r):
        rows = [jnp.broadcast_to(ref[r, layer, hd:hd + 1, :], (128, HD)).T for hd in range(GH)]
        col = jnp.concatenate(rows, 0)
        return jnp.concatenate([col] * (TT // 128), 1)

    def project_qkv(layer, n):
        r, tile, b = n // 4, lax.rem(n, 4), 0
        rows = pl.ds(pl.multiple_of(tile * TT, TT), TT)
        cols = pl.ds(pl.multiple_of(r * 2 * HW, 2 * HW), 2 * HW)
        t = dot(u[0:3 * GF, cols], h[rows, :], NT)
        qkv_at(b, 0, GF)[...] = (t[:GF] + column(hid[0], layer, r)).astype(BF16)
        qkv_at(b, GF, GF)[...] = t[GF:2 * GF].astype(BF16)
        t = (t[2 * GF:] + column(hid[1], layer, r)).astype(BF16)
        for hd in range(GH):
            qkv_at(b, 2 * GF + hd * VR, HD)[...] = t[hd * HD:(hd + 1) * HD, :]

    def heads(n):
        r, tile, b = n // 4, lax.rem(n, 4), 0
        score, weigh, value = [], [], []
        for img in range(TT // NTOK):
            c = slice(img * NTOK, (img + 1) * NTOK)
            for hd in range(GH):
                box = {}

                def f(hd=hd, c=c, box=box):
                    qt = qkv_at(b, hd * HD, HD)[:, c]
                    kt = qkv_at(b, GF + hd * HD, HD)[:, c]
                    box["s"] = dot(kt, qt, TN)

                def g(box=box):
                    st = box["s"]
                    box["e"] = jnp.exp2((st - jnp.max(st, 0, keepdims=True)) * scale).astype(BF16)

                def w(hd=hd, c=c, img=img, box=box):
                    t = dot(qkv_at(b, 2 * GF + hd * VR, VR)[:, c], box["e"])
                    at = pl.ds(pl.multiple_of(tile * 4 * GF + r * GF + hd * HD, 16), HD)
                    dbuf[img, at, :] = (t[:HD] * (1.0 / t[HD:HD + 1])).astype(BF16)
                score.append(f)
                weigh.append(g)
                value.append(w)
        return score, weigh, value

    def run_heads(n):
        score, weigh, value = heads(n)
        for f in score:
            f()
        for g, w in zip(weigh, value):
            g()
            w()

    def project_block(layer, tile):
        b0, b1 = vec_row(layer, 2)
        at = pl.ds(pl.multiple_of(tile * 4 * GF, 4 * GF), 4 * GF)
        o = jnp.concatenate([dbuf[img, at, :].T for img in range(TT // NTOK)], 0)
        rows = pl.ds(pl.multiple_of(tile * TT, TT), TT)
        for half, ref, bias in ((0, x0, b0), (1, x1, b1)):
            acc = dot(o[:, :HW], u[3 * GF:5 * GF, half * HW:(half + 1) * HW])
            acc += dot(o[:, HW:], u[3 * GF:5 * GF, 2 * HW + half * HW:2 * HW + (half + 1) * HW])
            ref[rows, :] = (ref[rows, :].astype(F32) + acc + bias).astype(BF16)

    def up_block(layer, k, tile, b):
        rows = pl.ds(pl.multiple_of(tile * TT, TT), TT)
        bias = jnp.concatenate(
            [hid[2][r, layer:layer + 1, pl.ds(pl.multiple_of(k * UC, 128), UC)] for r in range(4)], 1)
        for first in range(0, 4 * UC, NB):
            t = gelu(dot(h[rows, :], big[pl.ds(pl.multiple_of((2 + b) * TOKENS, TOKENS), 2 * HW), first:first + NB]) + bias[:, first:first + NB]).astype(BF16)
            at = first
            while at < first + NB:
                r, off = divmod(at, UC)
                size = min(UC - off, first + NB - at)
                u[rows, pl.ds(pl.multiple_of(r * FB + k * UC + off, 128), size)] = t[:, at - first:at - first + size]
                at += size

    def down_block(layer, cc, tile, b):
        rows = pl.ds(pl.multiple_of(tile * TT, TT), TT)
        cols = pl.ds(pl.multiple_of(cc * DC, DC), DC)
        acc = dot(u[rows, :], dbuf[b])
        for half, ref, vec in ((0, x0, vec_own[5]), (1, x1, vec_oth[5])):
            new = ref[rows, cols].astype(F32) + acc[:, half * DC:(half + 1) * DC] + vec[layer:layer + 1, cols]
            ref[rows, cols] = new.astype(BF16)

    program, _, _ = plan()
    before = {}
    todo = []
    tail = []
    for item in program:
        if item[0] == "do":
            todo.append(item[1])
        else:
            before[item[1:]] = todo
            todo = []
    tail = todo

    def ahead(layer, kind, n, first=0):
        def branch(some):
            if len(some) == 1:
                for a in before[(layer, kind, some[0])] if some[0] >= first else ():
                    act(a)
                return
            half = len(some) // 2

            @pl.when(n < some[half])
            def _():
                branch(some[:half])

            @pl.when(n >= some[half])
            def _():
                branch(some[half:])

        branch(range(BLOCKS[kind]))

    def straight(layer, kind, n):
        for a in before[(layer, kind, n)]:
            act(a)

    def at_loads(n, count, wait):
        for j in range(count):
            @pl.when(n == j * TILES)
            def _(j=j):
                wait(j)

    def norm_first(layer, tile):
        if layer == 0:
            whole(x1.at[tile * TT:(tile + 1) * TT, :], irecv.at[tile])
        norm(layer, 0, tile)

    for layer in range(LAYERS):
        straight(layer, "a", 0)
        if layer == 0:
            for j in range(3):
                hid_copy(j, X).wait_recv()
                hid_copy(j, XC).start()
            for j in range(3):
                hid_copy(j, C).wait_recv()
                hid_copy(j, XC).wait_recv()
                hid[j][0] = hid_own[j][...]
            for j in range(6):
                vec_copy(j).wait_recv()
            loaded(x0, local_sem.at[0])
        ones_rows()

        @pl.loop(0, 4 * TILES)
        def _(n, layer=layer):
            ahead(layer, "a", n, 1)
            for r in range(4):
                @pl.when(n == 4 * r)
                def _(r=r):
                    a_loaded(r)
            for tile in range(TILES):
                @pl.when(n == tile)
                def _(tile=tile):
                    norm_first(layer, tile)
            project_qkv(layer, n)

            @pl.when(n < BLOCKS["a"])
            def _():
                run_heads(n)

        @pl.loop(0, TILES)
        def _(n, layer=layer):
            ahead(layer, "p", n)

            @pl.when(n == 0)
            def _():
                o_loaded()
            project_block(layer, n)
            norm(layer, 3, n)

        @pl.loop(0, NU * TILES)
        def _(n, layer=layer):
            ahead(layer, "u", n)
            k, tile = n // TILES, lax.rem(n, TILES)
            at_loads(n, NU, u_loaded)
            up_block(layer, k, tile, lax.rem(k, 2))

        @pl.loop(0, ND * TILES)
        def _(n, layer=layer):
            ahead(layer, "d", n)
            cc, tile = n // TILES, lax.rem(n, TILES)
            at_loads(n, ND, d_loaded)
            down_block(layer, cc, tile, lax.rem(cc, DB))

    def sent(ref, sem):
        remote(ref, ref, sem, irecv.at[0], over_c).wait_send()

    for s in range(7):
        sent(land_a.at[0, 0:6], wsend.at[s])
    sent(x1, isend.at[0])
    for j in range(6):
        vec_copy(j).wait_send()
    for j in range(3):
        for s in (X, C, XC):
            hid_copy(j, s).wait_send()
    for a in tail:
        act(a)
    whole(big.at[0:2 * TOKENS, :], osend.at[7])
    for s in range(7):
        sent(x1, osend.at[s])


def mega(x_in, wq, wk, wv, wo, wup, wdown, *small):
    any_spec = pl.BlockSpec(memory_space=pl.ANY)
    vm = pl.BlockSpec(memory_space=pltpu.VMEM)
    dma = pltpu.SemaphoreType.DMA
    shapes = ((LAYERS, 7, 4 * GF, HW), (LAYERS, 7, HW, FB), (LAYERS, 7, FB, HW))
    flops = 2 * TOKENS * FB * 16384 * LAYERS
    return pl.pallas_call(
        mega_kernel,
        out_shape=(pltpu.VMEM((4 * TOKENS, 2 * HW), BF16),) + tuple(jax.ShapeDtypeStruct(s, BF16) for s in shapes),
        in_specs=[any_spec] * 7 + [vm] * 9,
        out_specs=[vm] + [any_spec] * 3,
        scratch_shapes=[
            pltpu.VMEM((TOKENS, HW), BF16), pltpu.VMEM((TOKENS, 4 * FB), BF16),
            pltpu.VMEM((DB, 4 * FB, 2 * DC), BF16), pltpu.VMEM((2 * GF + GH * VR, TT), BF16),
            *[pltpu.VMEM(a.shape, F32) for a in small[:6]], *[pltpu.VMEM((4,) + a.shape, F32) for a in small[6:]],
            dma((7,)), dma((LAYERS * (NU + ND), 4)), dma((LAYERS * NA, 3)), dma((LAYERS, 5)),
            dma((1,)), dma((TILES,)), dma((8,)), dma((UNITS, 3)),
            dma((15,)), dma((15,)), dma((1,)), dma((5,)), dma((2,)), dma((DB,)), pltpu.SemaphoreType.REGULAR,
        ],
        compiler_params=pltpu.CompilerParams(collective_id=0, has_side_effects=True, vmem_limit_bytes=41000000),
        cost_estimate=pl.CostEstimate(flops=flops, bytes_accessed=300 << 20, transcendentals=0),
        name="encoder",
    )(x_in, wq, wk, wv, wo, wup, wdown, *small)[0]


def hand_over(big, shape):
    def copy(big_ref, out_ref, sem):
        me = lax.axis_index("tx") * 4 + lax.axis_index("ty")
        copies = []
        for s in range(8):
            place = sum(((me // bit + s // bit) % 2) * bit for bit in (1, 2, 4))
            for i in range(IMGS):
                row, col = (s // 2) * TOKENS + i * NTOK, (s % 2) * HW
                copies.append(pltpu.make_async_copy(
                    big_ref.at[row:row + NTOK, col:col + HW], out_ref.at[place * IMGS + i], sem))
        for c in copies:
            c.start()
        pltpu.make_async_copy(out_ref, out_ref, sem).wait()

    return pl.pallas_call(
        copy, out_shape=jax.ShapeDtypeStruct(shape, big.dtype),
        in_specs=[pl.BlockSpec(memory_space=pltpu.VMEM)], out_specs=pl.BlockSpec(memory_space=pl.ANY),
        scratch_shapes=[pltpu.SemaphoreType.DMA],
        compiler_params=pltpu.CompilerParams(vmem_limit_bytes=1 << 20), name="hand_over")(big)


def solution(mesh):
    act_spec = P("dp", None, "tx")
    vec_tx = P(None, "tx")
    proj_spec = P(None, "tx", "ty", None)
    head_vec = P(None, "ty", None)
    in_specs = (act_spec, vec_tx, vec_tx, proj_spec, head_vec, proj_spec, proj_spec, head_vec,
                P(None, "ty", None, "tx"), vec_tx, vec_tx, vec_tx,
                P(None, "tx", "ty"), P(None, "ty"), P(None, "ty", "tx"), vec_tx)

    def heads_first(w):
        return jnp.transpose(w, (0, 2, 3, 1)).reshape(LAYERS, GF, HW)

    def local_fn(x_in, ln1_gain, ln1_bias, w_q, b_q, w_k, w_v, b_v, w_o, b_o, ln2_gain, ln2_bias, w_up, b_up, w_down, b_down):
        big = mega(x_in, heads_first(w_q), heads_first(w_k), heads_first(w_v), w_o.reshape(LAYERS, GF, HW), w_up, w_down,
                   ln1_gain, ln1_bias, b_o, ln2_gain, ln2_bias, b_down, b_q, b_v, b_up)
        return hand_over(big, x_in.shape)

    return jax.shard_map(local_fn, mesh=mesh, in_specs=in_specs, out_specs=act_spec, check_vma=False)
```

```python
import math

import jax
import jax.numpy as jnp
from jax import lax
from jax.experimental import pallas as pl
from jax.experimental.pallas import tpu as pltpu
from jax.sharding import PartitionSpec as P

EPS = 1e-6
F32 = jnp.float32
BF16 = jnp.bfloat16
MESH = pl.DeviceIdType.MESH

IMGS = 8
NTOK = 256
TOKENS = IMGS * NTOK
TILES = 4
TT = 512
HD = 96
GH = 4
GF = GH * HD
HW = 768
FB = 1536
UC = 384
DC = 128
NA, NU = 4, 4
ND = 6
DB = 2
PER_LAYER = NA + NU + ND
LAYERS = 2
CHUNKS = LAYERS * PER_LAYER
UNITS = ND * TILES
NB = 768
VR = HD + 16

X, Y, C = 2, 4, 1
XC, YC, XY, XYC = 3, 5, 6, 7

NN = (((1,), (0,)), ((), ()))
NT = (((1,), (1,)), ((), ()))
TN = (((0,), (0,)), ((), ()))


def dot(a, b, dims=NN):
    return lax.dot_general(a, b, dims, preferred_element_type=F32)


def gelu(x):
    return 0.5 * x * (1.0 + jnp.tanh(x * (0.7978845608028654 + 0.035677408136300125 * (x * x))))


def chunk_kind(k):
    layer, j = divmod(k, PER_LAYER)
    if j < NA:
        return layer, "a", j
    if j < NA + NU:
        return layer, "u", j - NA
    return layer, "d", j - NA - NU


LINK = 46.6e3
BACKLOG = 12.0
MODES = "yxxyxxxxxxyxxxyyyxxyyxyyyyyy"
RANK_X = "uuruyvywnqtqqskjnmuqoonqomqo"
RANK_Y = "gjhgpqqoiiiighdedgecaenonmkl"
RANK_R = "oqpmsvvtqooqssgieilnoqnlnlln"
RANK_I = "ntkhrrlh"
EARLY, OUTS = -17, 4
AROUND = 3
BLOCKS = {"a": 16, "p": TILES, "u": NU * TILES, "d": ND * TILES}


def behind(letter):
    return 5 * (ord(letter) - ord("m"))


def relay_on_x(k):
    return MODES[k] == "x"


def chunk_bytes(k):
    return 2 * (FB * DC if chunk_kind(k)[1] == "d" else GF * HW)


def block_cost(kind, n):
    if kind == "a":
        return 3.06 + (1.25 if n < 4 else 0.0)
    return {"p": 3.87, "u": 3.16, "d": 46.0 / (ND * TILES)}[kind]


def plan():
    free = {"x": 0.0, "y": 0.0, "c": 0.0}
    ready = {}
    pending = []
    program = []
    now = [4.5]
    queue = {"x": [(10 * k + behind(RANK_X[k]), ("ownx", k)) for k in range(CHUNKS)],
             "y": [(10 * k + behind(RANK_Y[k]), ("owny", k)) for k in range(CHUNKS)]
             + [(20 + 3 * i + behind(RANK_I[i]), ("image", i)) for i in range(IMGS)]}
    given = set()
    passed = {None}
    unit = TT * DC * 2

    def send(link, size):
        rate, lag = (450e3, 1.5) if link == "c" else (LINK, 2.5)
        free[link] = max(free[link], now[0]) + size / rate
        return free[link] + lag

    def arrive(name, time, action=None):
        ready[name] = time
        if action is not None:
            pending.append((time, action))

    loads = []
    for layer in range(LAYERS):
        base = layer * PER_LAYER
        old = (layer - 1, "d", BLOCKS["d"] - 1) if layer else None
        for r in range(4):
            loads.append((("la", layer, r), [("w", s, base + j) for s in (r, 4 + r) if s for j in range(3)], old, 1.9))
        loads.append((("lo", layer), [("w", s, base + 3) for s in range(1, 8)], old, 2.2))
        for k in range(NU):
            last = (layer, "u", (k - 2) * TILES + TILES - 1) if k > 1 else old and (layer - 1, "u", BLOCKS["u"] - 1)
            loads.append((("lu", layer, k), [("w", s, base + NA + k) for s in range(1, 6)], last, 1.8))
            loads.append((("mu", layer, k), [("w", s, base + NA + k) for s in (XY, XYC)], last, 1.1))
        for j in range(ND):
            last = (layer, "d", (j - DB) * TILES + TILES - 1) if j >= DB else (layer, "p", TILES - 1)
            loads.append((("ld", layer, j), [("w", s, base + NA + NU + j) for s in range(1, 6)], last, 1.5))
            loads.append((("md", layer, j), [("w", s, base + NA + NU + j) for s in (XY, XYC)], last, 1.0))

    def do(action):
        program.append(("do", action))
        kind, *k = action
        k = k[0] if k else None
        if kind == "ownx":
            arrive(("w", X, k), send("x", chunk_bytes(k)), ("gotx", k))
        elif kind == "owny":
            arrive(("w", Y, k), send("y", chunk_bytes(k)), ("goty", k))
        elif kind == "ownc":
            arrive(("w", C, k), send("c", chunk_bytes(k)))
        elif kind == "image":
            arrive(("image", k), send("y", NTOK * HW * 2))
        elif kind == "gotx":
            arrive(("w", XC, k), send("c", chunk_bytes(k)))
            if not relay_on_x(k):
                queue["y"].append((10 * k + behind(RANK_R[k]), ("relay", k)))
        elif kind == "goty":
            arrive(("w", YC, k), send("c", chunk_bytes(k)))
            if relay_on_x(k):
                queue["x"].append((10 * k + behind(RANK_R[k]), ("relay", k)))
        elif kind == "relay":
            arrive(("w", XY, k), send("x" if relay_on_x(k) else "y", chunk_bytes(k)), ("gotd", k))
        elif kind == "gotd":
            arrive(("w", XYC, k), send("c", chunk_bytes(k)))
        elif kind == "out":
            queue["y"].append((10 * CHUNKS - EARLY + OUTS * k, ("outp", k)))
            arrive(("o", X, k), send("x", unit), ("outx", k))
            arrive(("o", C, k), send("c", unit))
            if k < AROUND:
                arrive(("z", k), send("x", unit), ("pass", k))
        elif kind == "pass":
            queue["y"].append((20 * CHUNKS + k, ("passy", k)))
        elif kind == "passy":
            arrive(("o", XY, k), send("y", unit), ("outd", k))
        elif kind == "outp":
            arrive(("o", Y, k), send("y", unit), ("outy", k))
        elif kind == "outx":
            arrive(("o", XC, k), send("c", unit))
        elif kind == "outy":
            if k >= AROUND:
                arrive(("o", XY, k), send("x", unit), ("outd", k))
            arrive(("o", YC, k), send("c", unit))
        elif kind == "outd":
            arrive(("o", XYC, k), send("c", unit))

    def pump():
        while True:
            due = [p for p in pending if p[0] <= now[0]]
            if due:
                first = min(due)
                pending.remove(first)
                do(first[1])
                continue
            for link in ("y", "x"):
                if queue[link] and free[link] - now[0] < BACKLOG:
                    first = min(queue[link])
                    queue[link].remove(first)
                    do(first[1])
                    if first[1][0] in ("ownx", "owny") and first[1][1] not in given:
                        given.add(first[1][1])
                        do(("ownc", first[1][1]))
                    break
            else:
                break
        for load in list(loads):
            action, needs, last, cost = load
            if last in passed and all(ready.get(a, 1e9) <= now[0] for a in needs):
                loads.remove(load)
                program.append(("do", action))
                ready[action] = now[0] + cost

    def block(layer, kind, n, needs, cost):
        while True:
            pump()
            late = [ready.get(a, 1e9) for a in needs if ready.get(a, 1e9) > now[0]]
            if not late:
                break
            times = [p[0] for p in pending] + [t for t in ready.values() if t > now[0]]
            times += [free[link] - BACKLOG + 1e-6 for link in queue if queue[link]]
            now[0] = max(now[0], min(times))
        program.append(("block", layer, kind, n))
        passed.add((layer, kind, n))
        now[0] += cost

    mark = []
    do(("small",))
    pump()
    for layer in range(LAYERS):
        for n in range(BLOCKS["a"]):
            needs = [("la", layer, n // 4)]
            if layer == 0 and n < 4:
                needs += [("image", 2 * n), ("image", 2 * n + 1)]
            block(layer, "a", n, needs, block_cost("a", n))
        for n in range(TILES):
            block(layer, "p", n, [("lo", layer)], block_cost("p", n))
        for n in range(BLOCKS["u"]):
            block(layer, "u", n, [("lu", layer, n // TILES), ("mu", layer, n // TILES)], block_cost("u", n))
        for n in range(BLOCKS["d"]):
            if layer == LAYERS - 1 and n == 0:
                do(("leave",))
            block(layer, "d", n, [("ld", layer, n // TILES), ("md", layer, n // TILES)], block_cost("d", n))
            mark.append(now[0])
            if layer == LAYERS - 1:
                do(("out", n))
    while pending or queue["y"]:
        times = [p[0] for p in pending] + [free["y"] - BACKLOG + 1e-6 for _ in queue["y"]]
        now[0] = max(now[0], min(times))
        pump()
    return program, max(now[0], max(ready.values())), mark


def mega_kernel(x_in, wq, wk, wv, wo, wup, wdown, *rest):
    vec_own, hid_own, rest = rest[:6], rest[6:9], rest[9:]
    big, land_a, land_u, land_d, x1, u, dbuf, qkv = rest[:8]
    vec_oth, hid, rest = rest[8:14], rest[14:17], rest[17:]
    encoder_body(x_in, wq, wk, wv, wo, wup, wdown, vec_own, hid_own, big, land_a, land_u, land_d,
                 x1, u, dbuf, qkv, vec_oth, hid, *rest)


def encoder_body(x_in, wq, wk, wv, wo, wup, wdown, vec_own, hid_own, big, land_a, land_u, land_d,
                 x1, u, dbuf, qkv, vec_oth, hid,
                wsend, wrecv, arecv, crecv, isend, irecv, osend, orecv, small_send, small_recv,
                local_sem, asem, usem, dsem, zsend, zrecv, credit):
    ty, tx = lax.axis_index("ty"), lax.axis_index("tx")
    core, xx = lax.rem(ty, 2), ty // 2
    me = tx * 4 + ty
    x0 = big.at[0:TOKENS, 0:HW]
    h = big.at[TOKENS:2 * TOKENS, :]
    over_x = {"ty": (1 - xx) * 2 + core}
    over_y = {"tx": 1 - tx}
    over_c = {"ty": xx * 2 + (1 - core)}
    src_wa = (wq, wk, wv, wo)

    barrier = pltpu.get_barrier_semaphore()
    for peer in (over_x, over_y, over_c):
        pl.semaphore_signal(barrier, inc=1, device_id=peer, device_id_type=MESH)
    pl.semaphore_wait(barrier, 3)

    def remote(src, dst, send, recv, peer):
        return pltpu.make_async_remote_copy(src_ref=src, dst_ref=dst, send_sem=send, recv_sem=recv,
                                            device_id=peer, device_id_type=MESH)

    def own_ref(k):
        layer, kind, j = chunk_kind(k)
        if kind == "a":
            return src_wa[j].at[layer]
        if kind == "u":
            return wup.at[layer, :, j * UC:(j + 1) * UC]
        return wdown.at[layer, :, j * DC:(j + 1) * DC]

    def land_ref(k, s):
        layer, kind, j = chunk_kind(k)
        if kind == "a":
            return land_a.at[layer, s - 1, j * GF:(j + 1) * GF, :]
        if kind == "u":
            return land_u.at[layer, s - 1, :, j * UC:(j + 1) * UC]
        return land_d.at[layer, s - 1, :, j * DC:(j + 1) * DC]

    def weight_copy(k, s):
        if s == X:
            src, peer = own_ref(k), over_x
        elif s == Y:
            src, peer = own_ref(k), over_y
        elif s == C:
            src, peer = own_ref(k), over_c
        elif s == XY:
            src, peer = (land_ref(k, Y), over_x) if relay_on_x(k) else (land_ref(k, X), over_y)
        else:
            src, peer = land_ref(k, s - 1), over_c
        return remote(src, land_ref(k, s), wsend.at[s - 1], landed(k, s), peer)

    def landed(k, s):
        layer, kind, j = chunk_kind(k)
        hop = (X, Y, XY).index(s) if s in (X, Y, XY) else 4 if s == XYC and kind != "a" else 3
        if kind != "a":
            return wrecv.at[k - (layer + 1) * NA, hop]
        if hop < 3:
            return arecv.at[layer * NA + j, hop]
        return crecv.at[layer, 4 if j == 3 else s // 2]

    def whole(ref, sem):
        return remote(ref, ref, wsend.at[0], sem, over_c).wait_recv()

    def image_copy(i):
        theirs = (1 - tx) * 4 + ty
        return remote(x_in.at[theirs * IMGS + i], x1.at[i * NTOK:(i + 1) * NTOK, :], isend.at[0], irecv.at[i // 2], over_y)

    def out_ref(s, q):
        cc, i = divmod(q, TILES)
        row, col = (s // 2) * TOKENS + i * TT, (s % 2) * HW + cc * DC
        return big.at[row:row + TT, col:col + DC]

    def aside(q):
        return qkv.at[q // 4 * TT:(q // 4 + 1) * TT, q % 4 * DC:(q % 4 + 1) * DC]

    def aside_copy(q):
        cc, i = divmod(q, TILES)
        src = x1.at[i * TT:(i + 1) * TT, cc * DC:(cc + 1) * DC]
        return remote(src, aside(q), zsend.at[q], zrecv.at[q], over_x)

    def out_copy(q, s):
        cc, i = divmod(q, TILES)
        if s == X:
            src, peer = out_ref(0, q), over_x
        elif s == C:
            src, peer = out_ref(0, q), over_c
        elif s == Y:
            src, peer = x1.at[i * TT:(i + 1) * TT, cc * DC:(cc + 1) * DC], over_y
        elif s == XY:
            src, peer = (aside(q), over_y) if q < AROUND else (out_ref(Y, q), over_x)
        else:
            src, peer = out_ref(s - 1, q), over_c
        return remote(src, out_ref(s, q), osend.at[s - 1], left(q, s), peer)

    def left(q, s):
        return orecv.at[q, (X, Y, XY).index(s)] if s in (X, Y, XY) else osend.at[7]

    def out_arrived(q, s):
        return remote(out_ref(s, q), out_ref(s, q), osend.at[s - 1], left(q, s), over_x)

    def small(src, dst, j, peer):
        return remote(src, dst, small_send.at[j], small_recv.at[j], peer)

    def vec_copy(j):
        return small(vec_own[j], vec_oth[j], j, over_y)

    def hid_copy(j, s):
        src = hid[j].at[X] if s == XC else hid_own[j]
        return small(src, hid[j].at[s], 6 + 3 * j + s - 1, over_x if s == X else over_c)

    def own_rows(i):
        return pltpu.make_async_copy(x_in.at[me * IMGS + i], big.at[i * NTOK:(i + 1) * NTOK, 0:HW], local_sem.at[0])

    def act(action):
        kind, *k = action
        k = k[0] if k else None
        if kind == "small":
            for j in range(3):
                hid_copy(j, X).start()
            for j in range(3):
                hid_copy(j, C).start()
            for j in range(6):
                vec_copy(j).start()
            for i in range(IMGS):
                own_rows(i).start()
        elif kind == "ownx":
            weight_copy(k, X).start()
        elif kind == "owny":
            weight_copy(k, Y).start()
        elif kind == "ownc":
            weight_copy(k, C).start()
        elif kind == "image":
            image_copy(k).start()
        elif kind == "gotx":
            weight_copy(k, X).wait_recv()
            weight_copy(k, XC).start()
        elif kind == "goty":
            weight_copy(k, Y).wait_recv()
            weight_copy(k, YC).start()
        elif kind == "relay":
            weight_copy(k, XY).start()
        elif kind == "gotd":
            weight_copy(k, XY).wait_recv()
            weight_copy(k, XYC).start()
        elif kind == "out":
            if k == 0:
                pl.semaphore_wait(credit, 3)
            for s in (X, C):
                out_copy(k, s).start()
            if k < AROUND:
                aside_copy(k).start()
        elif kind == "pass":
            aside_copy(k).wait_recv()
        elif kind == "passy":
            out_copy(k, XY).start()
        elif kind == "outp":
            out_copy(k, Y).start()
        elif kind == "leave":
            for peer in (over_x, over_y, over_c):
                pl.semaphore_signal(credit, inc=1, device_id=peer, device_id_type=MESH)
        elif kind == "outx":
            out_arrived(k, X).wait_recv()
            out_copy(k, XC).start()
        elif kind == "outy":
            out_arrived(k, Y).wait_recv()
            if k >= AROUND:
                out_copy(k, XY).start()
            out_copy(k, YC).start()
        elif kind == "outd":
            out_arrived(k, XY).wait_recv()
            out_copy(k, XYC).start()
        elif kind == "la":
            layer, r = action[1:]
            for s in (r, 4 + r):
                if s % 2:
                    whole(land_a.at[layer, s - 1, 0:3 * GF, :], crecv.at[layer, s // 2])
            start(a_loads(layer, r))
        elif kind == "lo":
            arrived(action[1] * PER_LAYER + 3)
            start(o_loads(action[1]))
        elif kind == "lu":
            arrived(action[1] * PER_LAYER + NA + action[2])
            start(u_loads(*action[1:])[:6])
        elif kind == "ld":
            arrived(action[1] * PER_LAYER + NA + NU + action[2])
            start(d_loads(*action[1:])[:6])
        elif kind == "mu":
            weight_copy(action[1] * PER_LAYER + NA + action[2], XYC).wait_recv()
            start(u_loads(*action[1:])[6:])
        elif kind == "md":
            weight_copy(action[1] * PER_LAYER + NA + NU + action[2], XYC).wait_recv()
            start(d_loads(*action[1:])[6:])

    def slot_ref(land, own, layer, s):
        return own.at[layer] if s == 0 else land.at[layer, s - 1]

    def a_loads(layer, r):
        out = []
        for dy in range(2):
            s = dy * 4 + r
            cols = slice(r * 2 * HW + dy * HW, r * 2 * HW + (dy + 1) * HW)
            if s == 0:
                for j in range(3):
                    out.append((src_wa[j].at[layer], u.at[j * GF:(j + 1) * GF, cols], asem.at[r]))
            else:
                out.append((land_a.at[layer, s - 1, 0:3 * GF, :], u.at[0:3 * GF, cols], asem.at[r]))
        return [pltpu.make_async_copy(*c) for c in out]

    def o_loads(layer):
        out = []
        for r in range(4):
            for dy in range(2):
                s = dy * 4 + r
                src = wo.at[layer] if s == 0 else land_a.at[layer, s - 1, 3 * GF:4 * GF, :]
                at = 3 * GF + (r % 2) * GF
                cols = slice((r // 2) * 2 * HW + dy * HW, (r // 2) * 2 * HW + (dy + 1) * HW)
                out.append(pltpu.make_async_copy(src, u.at[at:at + GF, cols], asem.at[4]))
        return out

    def u_loads(layer, k):
        b = k % 2
        out = []
        for dy in range(2):
            for r in range(4):
                s = dy * 4 + r
                src = slot_ref(land_u, wup, layer, s).at[:, k * UC:(k + 1) * UC]
                out.append(pltpu.make_async_copy(
                    src, big.at[(2 + b) * TOKENS + dy * HW:(2 + b) * TOKENS + (dy + 1) * HW, r * UC:(r + 1) * UC], usem.at[b]))
        return out

    def d_loads(layer, cc):
        b = cc % DB
        out = []
        for dy in range(2):
            for r in range(4):
                s = dy * 4 + r
                src = slot_ref(land_d, wdown, layer, s).at[:, cc * DC:(cc + 1) * DC]
                out.append(pltpu.make_async_copy(
                    src, dbuf.at[b, r * FB:(r + 1) * FB, dy * DC:(dy + 1) * DC], dsem.at[b]))
        return out

    def start(copies):
        for c in copies:
            c.start()

    def loaded(ref, sem):
        pltpu.make_async_copy(ref, ref, sem).wait()

    def a_loaded(r):
        loaded(u.at[0:3 * GF, r * 2 * HW:(r + 1) * 2 * HW], asem.at[r])

    def o_loaded():
        loaded(u.at[3 * GF:5 * GF, 0:4 * HW], asem.at[4])

    def u_loaded(k):
        at = (2 + k % 2) * TOKENS
        loaded(big.at[at:at + 2 * HW, :], usem.at[k % 2])

    def d_loaded(cc):
        loaded(dbuf.at[cc % DB], dsem.at[cc % DB])

    def arrived(k):
        layer, kind, j = chunk_kind(k)
        if kind == "a":
            ref = land_a.at[layer, 0:4, j * GF:(j + 1) * GF, :]
        elif kind == "u":
            ref = land_u.at[layer, 0:3, :, j * UC:(j + 1) * UC]
        else:
            ref = land_d.at[layer, 0:3, :, j * DC:(j + 1) * DC]
        whole(ref, landed(k, C))

    def vec_row(layer, j):
        return vec_own[j][layer:layer + 1, :], vec_oth[j][layer:layer + 1, :]

    def norm(layer, j, tile):
        g0, g1 = vec_row(layer, j)
        s0, s1 = vec_row(layer, j + 1)
        rows, group = 16, 8

        @pl.loop(0, TT // (rows * group))
        def _(i):
            ats = [pl.ds(pl.multiple_of(tile * TT + (i * group + m) * rows, rows), rows) for m in range(group)]
            pairs = [(x0[at, :].astype(F32), x1[at, :].astype(F32)) for at in ats]
            done = []
            for a, b in pairs:
                mean = jnp.sum(a + b, 1, keepdims=True) * (0.5 / HW)
                a = a - mean
                b = b - mean
                var = jnp.sum(a * a + b * b, 1, keepdims=True) * (0.5 / HW)
                inv = lax.rsqrt(var + EPS)
                done.append(((a * inv * g0 + s0).astype(BF16), (b * inv * g1 + s1).astype(BF16)))
            for at, (a, b) in zip(ats, done):
                h[at, :HW] = a
                h[at, HW:] = b

    scale = HD ** -0.5 * math.log2(math.e)

    def qkv_at(b, first, rows):
        return qkv.at[first:first + rows, :]

    def ones_rows():
        for hd in range(GH):
            qkv_at(0, 2 * GF + hd * VR + HD, 16)[...] = jnp.ones((16, TT), BF16)

    def column(ref, layer, r):
        rows = [jnp.broadcast_to(ref[r, layer, hd:hd + 1, :], (128, HD)).T for hd in range(GH)]
        col = jnp.concatenate(rows, 0)
        return jnp.concatenate([col] * (TT // 128), 1)

    def project_qkv(layer, n):
        r, tile, b = n // 4, lax.rem(n, 4), 0
        rows = pl.ds(pl.multiple_of(tile * TT, TT), TT)
        cols = pl.ds(pl.multiple_of(r * 2 * HW, 2 * HW), 2 * HW)
        t = dot(u[0:3 * GF, cols], h[rows, :], NT)
        qkv_at(b, 0, GF)[...] = (t[:GF] + column(hid[0], layer, r)).astype(BF16)
        qkv_at(b, GF, GF)[...] = t[GF:2 * GF].astype(BF16)
        t = (t[2 * GF:] + column(hid[1], layer, r)).astype(BF16)
        for hd in range(GH):
            qkv_at(b, 2 * GF + hd * VR, HD)[...] = t[hd * HD:(hd + 1) * HD, :]

    def heads(n):
        r, tile, b = n // 4, lax.rem(n, 4), 0
        score, weigh, value = [], [], []
        for img in range(TT // NTOK):
            c = slice(img * NTOK, (img + 1) * NTOK)
            for hd in range(GH):
                box = {}

                def f(hd=hd, c=c, box=box):
                    qt = qkv_at(b, hd * HD, HD)[:, c]
                    kt = qkv_at(b, GF + hd * HD, HD)[:, c]
                    box["s"] = dot(kt, qt, TN)

                def g(box=box):
                    st = box["s"]
                    box["e"] = jnp.exp2((st - jnp.max(st, 0, keepdims=True)) * scale).astype(BF16)

                def w(hd=hd, c=c, img=img, box=box):
                    t = dot(qkv_at(b, 2 * GF + hd * VR, VR)[:, c], box["e"])
                    at = pl.ds(pl.multiple_of(tile * 4 * GF + r * GF + hd * HD, 16), HD)
                    dbuf[img, at, :] = (t[:HD] * (1.0 / t[HD:HD + 1])).astype(BF16)
                score.append(f)
                weigh.append(g)
                value.append(w)
        return score, weigh, value

    def run_heads(n):
        score, weigh, value = heads(n)
        for f in score:
            f()
        for g, w in zip(weigh, value):
            g()
            w()

    def project_block(layer, tile):
        b0, b1 = vec_row(layer, 2)
        at = pl.ds(pl.multiple_of(tile * 4 * GF, 4 * GF), 4 * GF)
        o = jnp.concatenate([dbuf[img, at, :].T for img in range(TT // NTOK)], 0)
        rows = pl.ds(pl.multiple_of(tile * TT, TT), TT)
        for half, ref, bias in ((0, x0, b0), (1, x1, b1)):
            acc = dot(o[:, :HW], u[3 * GF:5 * GF, half * HW:(half + 1) * HW])
            acc += dot(o[:, HW:], u[3 * GF:5 * GF, 2 * HW + half * HW:2 * HW + (half + 1) * HW])
            ref[rows, :] = (ref[rows, :].astype(F32) + acc + bias).astype(BF16)

    def up_block(layer, k, tile, b):
        rows = pl.ds(pl.multiple_of(tile * TT, TT), TT)
        bias = jnp.concatenate(
            [hid[2][r, layer:layer + 1, pl.ds(pl.multiple_of(k * UC, 128), UC)] for r in range(4)], 1)
        for first in range(0, 4 * UC, NB):
            t = gelu(dot(h[rows, :], big[pl.ds(pl.multiple_of((2 + b) * TOKENS, TOKENS), 2 * HW), first:first + NB]) + bias[:, first:first + NB]).astype(BF16)
            at = first
            while at < first + NB:
                r, off = divmod(at, UC)
                size = min(UC - off, first + NB - at)
                u[rows, pl.ds(pl.multiple_of(r * FB + k * UC + off, 128), size)] = t[:, at - first:at - first + size]
                at += size

    def down_block(layer, cc, tile, b):
        rows = pl.ds(pl.multiple_of(tile * TT, TT), TT)
        cols = pl.ds(pl.multiple_of(cc * DC, DC), DC)
        acc = dot(u[rows, :], dbuf[b])
        for half, ref, vec in ((0, x0, vec_own[5]), (1, x1, vec_oth[5])):
            new = ref[rows, cols].astype(F32) + acc[:, half * DC:(half + 1) * DC] + vec[layer:layer + 1, cols]
            ref[rows, cols] = new.astype(BF16)

    program, _, _ = plan()
    before = {}
    todo = []
    tail = []
    for item in program:
        if item[0] == "do":
            todo.append(item[1])
        else:
            before[item[1:]] = todo
            todo = []
    tail = todo

    def ahead(layer, kind, n, first=0):
        def branch(some):
            if len(some) == 1:
                for a in before[(layer, kind, some[0])] if some[0] >= first else ():
                    act(a)
                return
            half = len(some) // 2

            @pl.when(n < some[half])
            def _():
                branch(some[:half])

            @pl.when(n >= some[half])
            def _():
                branch(some[half:])

        branch(range(BLOCKS[kind]))

    def straight(layer, kind, n):
        for a in before[(layer, kind, n)]:
            act(a)

    def at_loads(n, count, wait):
        for j in range(count):
            @pl.when(n == j * TILES)
            def _(j=j):
                wait(j)

    def norm_first(layer, tile):
        if layer == 0:
            whole(x1.at[tile * TT:(tile + 1) * TT, :], irecv.at[tile])
        norm(layer, 0, tile)

    for layer in range(LAYERS):
        straight(layer, "a", 0)
        if layer == 0:
            for j in range(3):
                hid_copy(j, X).wait_recv()
                hid_copy(j, XC).start()
            for j in range(3):
                hid_copy(j, C).wait_recv()
                hid_copy(j, XC).wait_recv()
                hid[j][0] = hid_own[j][...]
            for j in range(6):
                vec_copy(j).wait_recv()
            loaded(x0, local_sem.at[0])
        ones_rows()

        @pl.loop(0, 4 * TILES)
        def _(n, layer=layer):
            ahead(layer, "a", n, 1)
            for r in range(4):
                @pl.when(n == 4 * r)
                def _(r=r):
                    a_loaded(r)
            for tile in range(TILES):
                @pl.when(n == tile)
                def _(tile=tile):
                    norm_first(layer, tile)
            project_qkv(layer, n)

            @pl.when(n < BLOCKS["a"])
            def _():
                run_heads(n)

        @pl.loop(0, TILES)
        def _(n, layer=layer):
            ahead(layer, "p", n)

            @pl.when(n == 0)
            def _():
                o_loaded()
            project_block(layer, n)
            norm(layer, 3, n)

        @pl.loop(0, NU * TILES)
        def _(n, layer=layer):
            ahead(layer, "u", n)
            k, tile = n // TILES, lax.rem(n, TILES)
            at_loads(n, NU, u_loaded)
            up_block(layer, k, tile, lax.rem(k, 2))

        @pl.loop(0, ND * TILES)
        def _(n, layer=layer):
            ahead(layer, "d", n)
            cc, tile = n // TILES, lax.rem(n, TILES)
            at_loads(n, ND, d_loaded)
            down_block(layer, cc, tile, lax.rem(cc, DB))

    def sent(ref, sem):
        remote(ref, ref, sem, irecv.at[0], over_c).wait_send()

    for s in range(7):
        sent(land_a.at[0, 0:6], wsend.at[s])
    sent(x1, isend.at[0])
    for j in range(6):
        vec_copy(j).wait_send()
    for j in range(3):
        for s in (X, C, XC):
            hid_copy(j, s).wait_send()
    for a in tail:
        act(a)
    for q in range(AROUND):
        aside_copy(q).wait_send()
    whole(big.at[0:2 * TOKENS, :], osend.at[7])
    for s in range(7):
        sent(x1, osend.at[s])


def mega(x_in, wq, wk, wv, wo, wup, wdown, *small):
    any_spec = pl.BlockSpec(memory_space=pl.ANY)
    vm = pl.BlockSpec(memory_space=pltpu.VMEM)
    dma = pltpu.SemaphoreType.DMA
    shapes = ((LAYERS, 7, 4 * GF, HW), (LAYERS, 7, HW, FB), (LAYERS, 7, FB, HW))
    flops = 2 * TOKENS * FB * 16384 * LAYERS
    return pl.pallas_call(
        mega_kernel,
        out_shape=(pltpu.VMEM((4 * TOKENS, 2 * HW), BF16),) + tuple(jax.ShapeDtypeStruct(s, BF16) for s in shapes),
        in_specs=[any_spec] * 7 + [vm] * 9,
        out_specs=[vm] + [any_spec] * 3,
        scratch_shapes=[
            pltpu.VMEM((TOKENS, HW), BF16), pltpu.VMEM((TOKENS, 4 * FB), BF16),
            pltpu.VMEM((DB, 4 * FB, 2 * DC), BF16), pltpu.VMEM((2 * GF + GH * VR, TT), BF16),
            *[pltpu.VMEM(a.shape, F32) for a in small[:6]], *[pltpu.VMEM((4,) + a.shape, F32) for a in small[6:]],
            dma((7,)), dma((LAYERS * (NU + ND), 5)), dma((LAYERS * NA, 3)), dma((LAYERS, 5)),
            dma((1,)), dma((TILES,)), dma((8,)), dma((UNITS, 3)),
            dma((15,)), dma((15,)), dma((1,)), dma((5,)), dma((2,)), dma((DB,)), dma((AROUND,)), dma((AROUND,)), pltpu.SemaphoreType.REGULAR,
        ],
        compiler_params=pltpu.CompilerParams(collective_id=0, has_side_effects=True, vmem_limit_bytes=41000000),
        cost_estimate=pl.CostEstimate(flops=flops, bytes_accessed=300 << 20, transcendentals=0),
        name="encoder",
    )(x_in, wq, wk, wv, wo, wup, wdown, *small)[0]


def hand_over(big, shape):
    def copy(big_ref, out_ref, sem):
        me = lax.axis_index("tx") * 4 + lax.axis_index("ty")
        copies = []
        for s in range(8):
            place = sum(((me // bit + s // bit) % 2) * bit for bit in (1, 2, 4))
            for i in range(IMGS):
                row, col = (s // 2) * TOKENS + i * NTOK, (s % 2) * HW
                copies.append(pltpu.make_async_copy(
                    big_ref.at[row:row + NTOK, col:col + HW], out_ref.at[place * IMGS + i], sem))
        for c in copies:
            c.start()
        pltpu.make_async_copy(out_ref, out_ref, sem).wait()

    return pl.pallas_call(
        copy, out_shape=jax.ShapeDtypeStruct(shape, big.dtype),
        in_specs=[pl.BlockSpec(memory_space=pltpu.VMEM)], out_specs=pl.BlockSpec(memory_space=pl.ANY),
        scratch_shapes=[pltpu.SemaphoreType.DMA],
        compiler_params=pltpu.CompilerParams(vmem_limit_bytes=1 << 20), name="hand_over")(big)


def solution(mesh):
    act_spec = P("dp", None, "tx")
    vec_tx = P(None, "tx")
    proj_spec = P(None, "tx", "ty", None)
    head_vec = P(None, "ty", None)
    in_specs = (act_spec, vec_tx, vec_tx, proj_spec, head_vec, proj_spec, proj_spec, head_vec,
                P(None, "ty", None, "tx"), vec_tx, vec_tx, vec_tx,
                P(None, "tx", "ty"), P(None, "ty"), P(None, "ty", "tx"), vec_tx)

    def heads_first(w):
        return jnp.transpose(w, (0, 2, 3, 1)).reshape(LAYERS, GF, HW)

    def local_fn(x_in, ln1_gain, ln1_bias, w_q, b_q, w_k, w_v, b_v, w_o, b_o, ln2_gain, ln2_bias, w_up, b_up, w_down, b_down):
        big = mega(x_in, heads_first(w_q), heads_first(w_k), heads_first(w_v), w_o.reshape(LAYERS, GF, HW), w_up, w_down,
                   ln1_gain, ln1_bias, b_o, ln2_gain, ln2_bias, b_down, b_q, b_v, b_up)
        return hand_over(big, x_in.shape)

    return jax.shard_map(local_fn, mesh=mesh, in_specs=in_specs, out_specs=act_spec, check_vma=False)
```
